32 devices in a mesh: ctx: 16 (over z, y, x), tp: 2 (over core).
Axes of the slice: x: 2, y: 2, z: 4, core: 2. Of those that a mesh axis runs over, the one named last changes fastest.
Arguments:
- byte_states: bfloat16 [4096, 1024], P('ctx'), may hold values from -12 to 12, as said below
- patch_of_byte: int32 [4096], P('ctx'), may hold values from 0 to 125, as said below
- patch_first: int32 [16], replicated, may hold values from 0 to 991, as said below
- moved: int32 [2, 16], replicated, may hold values from 0 to 32, as said below
- w_qkv: bfloat16 [3, 1024, 2048], P(None, None, 'tp'), may hold values from -0.25 to 0.25, as said below
- d_attn: bfloat16 [1024, 2048], P('ctx', 'tp'), may hold values from -6 to 6
Outputs:
- attn_out: bfloat16 [1024, 2048], P('ctx', 'tp')
- byte_grad: bfloat16 [4096, 1024], P('ctx', 'tp')
The draws below stay inside these ranges and needn't reach their ends.
Inputs may be any that keep to these rules, and one draw needn't show every extreme that they name: `patch_of_byte`: within each byte shard the numbers start at 0 and rise by 0 or 1 from byte to byte; a shard holds at most 126 patches, reached on some shard. `patch_first`: the sum of the patch counts of all earlier byte shards; shard 0 starts at 0. moved[0, 0] = 0 and moved[1, 15] = 0; every other entry is 1 to 32; every patch shard thereby receives exactly 64 patches, and the patch counts agree with patch_first and patch_of_byte. `w_qkv`: independent entries of order 1024 ** -0.5. `byte_states`: entries of order one.
All inputs are finite; a program needn't handle non-finite values.
Results may differ from the reference program's by a relative error of at most 0.011.
Values may be sent and summed in bfloat16 or wider, within the bound.
A program may use at most 64 MiB of HBM per device.

```python
import jax
import jax.numpy as jnp
from jax import lax

DL = 1024
HEADS = 16
HD = 128
P_DEV = 64
BYTE_DEV = 256
KEYS = 1024
BYTES = 4096
N_CTX = 16


def shard_plan(key):
    reach = P_DEV // 2
    lower_moves = jax.random.randint(jax.random.fold_in(key, 11), (N_CTX,), 1, reach + 1)
    upper_moves = jax.random.randint(jax.random.fold_in(key, 13), (N_CTX,), 1, reach + 1)
    chosen = jax.random.randint(jax.random.fold_in(key, 17), (), 1, N_CTX - 1)
    place = jnp.arange(N_CTX)
    lower_moves = jnp.where(place == chosen, reach, lower_moves)
    upper_moves = jnp.where(place == chosen, reach, upper_moves)
    upper_moves = jnp.where(place == chosen - 1, 1, upper_moves)
    lower_moves = jnp.where(place == chosen + 1, 1, lower_moves)
    lower_moves = jnp.where(place == 0, 0, lower_moves)
    upper_moves = jnp.where(place == N_CTX - 1, 0, upper_moves)
    below_high = jnp.concatenate([jnp.zeros((1,), jnp.int32), upper_moves[:-1]])
    above_low = jnp.concatenate([lower_moves[1:], jnp.zeros((1,), jnp.int32)])
    counts = P_DEV - below_high - above_low + lower_moves + upper_moves
    return (counts.astype(jnp.int32), lower_moves.astype(jnp.int32), upper_moves.astype(jnp.int32))


def draw_patch_first(key, part):
    counts, lower_moves, upper_moves = shard_plan(key)
    return (jnp.cumsum(counts) - counts).astype(jnp.int32)


def draw_moved(key, part):
    counts, lower_moves, upper_moves = shard_plan(key)
    return jnp.stack([lower_moves, upper_moves], axis=0).astype(jnp.int32)


def draw_patch_of_byte(key, part):
    counts, lower_moves, upper_moves = shard_plan(key)
    shard_keys = jax.random.split(jax.random.fold_in(key, 23), N_CTX)

    def one_shard(shard_key, count):
        order = jax.random.permutation(shard_key, BYTE_DEV - 1)
        cut = (order < count - 1).astype(jnp.int32)
        return jnp.concatenate([jnp.zeros((1,), jnp.int32), jnp.cumsum(cut).astype(jnp.int32)])
    return jax.vmap(one_shard)(shard_keys, counts).reshape(-1).astype(jnp.int32)


def draw_byte_states(key, part):
    values = jax.random.normal(key, (BYTES, DL), jnp.float32)
    return jnp.clip(values, -12.0, 12.0).astype(jnp.bfloat16)


def draw_w_qkv(key, part):
    values = jax.random.normal(key, (3, DL, HEADS * HD), jnp.float32) * DL ** (-0.5)
    return jnp.clip(values, -0.25, 0.25).astype(jnp.bfloat16)


def shard_levels(own_key, extent, cuts, least, top_value):
    level, own = 1.0, jax.random.fold_in(own_key, 6)
    for dim, parts in cuts:
        steps = jnp.exp(jax.random.uniform(jax.random.fold_in(own, dim), (parts,), jnp.float32, least / len(cuts), top_value / len(cuts)))
        level = level * jnp.repeat(steps, extent[dim] // parts).reshape([-1 if axis == dim else 1 for axis in range(len(extent))])
    return level


def scatter_about(own_key, extent, deviation, most, cuts=(), held_as=jnp.bfloat16):
    loudness = shard_levels(own_key, extent, cuts, -0.22, 0.18) if cuts else 1.0
    entries = jax.random.normal(own_key, extent, jnp.float32) * deviation * loudness
    return jnp.minimum(jnp.maximum(entries, -most), most).astype(held_as)


def setup_inputs(seed: int = 0) -> dict:
    key_list = jax.random.split(jax.random.key(seed), 7)
    return {
        "byte_states": draw_byte_states(jax.random.fold_in(key_list[6], 71), 0),
        "patch_of_byte": draw_patch_of_byte(jax.random.fold_in(key_list[6], 71), 0),
        "patch_first": draw_patch_first(jax.random.fold_in(key_list[6], 71), 0),
        "moved": draw_moved(jax.random.fold_in(key_list[6], 71), 0),
        "w_qkv": draw_w_qkv(jax.random.fold_in(key_list[6], 71), 0),
        "d_attn": scatter_about(key_list[5], (KEYS, HEADS * HD), 1.0, 6.0, ((0, 16), (1, 2))),
    }


def reference(byte_states, patch_of_byte, patch_first, moved, w_qkv, d_attn):
    shard = jnp.arange(BYTES, dtype=jnp.int32) // BYTE_DEV
    gid = (patch_first[shard] + patch_of_byte).astype(jnp.int32)
    sums = jax.ops.segment_sum(byte_states.astype(jnp.float32), gid, num_segments=KEYS)
    lengths = jax.ops.segment_sum(jnp.ones((BYTES,), jnp.float32), gid, num_segments=KEYS)
    pooled_global = (sums / lengths[:, None]).astype(jnp.bfloat16)

    place = jnp.arange(KEYS, dtype=jnp.int32)
    ends = jnp.concatenate([patch_first[1:], jnp.full((1,), KEYS, jnp.int32)]).astype(jnp.int32)
    counts = (ends - patch_first).astype(jnp.int32)
    lower_moves = moved[0]
    upper_moves = moved[1]
    below_high = jnp.concatenate([jnp.zeros((1,), jnp.int32), upper_moves[:-1]]).astype(jnp.int32)
    home = (jnp.sum((place[:, None] >= patch_first[None, :]).astype(jnp.int32), axis=1) - 1).astype(jnp.int32)
    local = (place - patch_first[home]).astype(jnp.int32)
    low_here = lower_moves[home]
    high_here = upper_moves[home]
    count_here = counts[home]
    goes_low = local < low_here
    goes_high = local >= count_here - high_here
    owner = jnp.where(goes_low, home - 1, jnp.where(goes_high, home + 1, home))
    rank = jnp.where(goes_low, P_DEV - low_here + local,
                     jnp.where(goes_high, local - (count_here - high_here), below_high[home] + local - low_here))
    slot = (owner * P_DEV + rank).astype(jnp.int32)
    order = jnp.zeros((KEYS,), jnp.int32).at[slot].set(place)

    pooled = pooled_global[order]
    query = jnp.dot(pooled, w_qkv[0], preferred_element_type=jnp.float32).astype(jnp.bfloat16)
    keyed = jnp.dot(pooled, w_qkv[1], preferred_element_type=jnp.float32).astype(jnp.bfloat16)
    valued = jnp.dot(pooled, w_qkv[2], preferred_element_type=jnp.float32).astype(jnp.bfloat16)
    scale = HD ** -0.5
    causal = order[:, None] >= order[None, :]

    def heads_first(x):
        return jnp.transpose(x.reshape(KEYS, HEADS, HD), (1, 0, 2))

    def per_head(items):
        q_head, k_head, v_head, g_head = items
        score = jnp.dot(q_head, k_head.T, preferred_element_type=jnp.float32) * scale
        masked = jnp.where(causal, score, -jnp.inf)
        top = jnp.max(masked, axis=1, keepdims=True)
        lse = top + jnp.log(jnp.sum(jnp.exp(masked - top), axis=1, keepdims=True))
        prob = jnp.exp(jnp.where(causal, score - lse, -jnp.inf))
        probs = prob.astype(jnp.bfloat16)
        output = jnp.dot(probs, v_head, preferred_element_type=jnp.float32).astype(jnp.bfloat16)
        delta = jnp.sum(g_head.astype(jnp.float32) * output.astype(jnp.float32), axis=1, keepdims=True)
        dprob = jnp.dot(g_head, v_head.T, preferred_element_type=jnp.float32)
        dscore = (prob * (dprob - delta)).astype(jnp.bfloat16)
        d_query = (jnp.dot(dscore, k_head, preferred_element_type=jnp.float32) * scale).astype(jnp.bfloat16)
        d_key = (jnp.dot(dscore.T, q_head, preferred_element_type=jnp.float32) * scale).astype(jnp.bfloat16)
        d_value = jnp.dot(probs.T, g_head, preferred_element_type=jnp.float32).astype(jnp.bfloat16)
        return output, d_query, d_key, d_value

    results = lax.map(per_head, (heads_first(query), heads_first(keyed), heads_first(valued), heads_first(d_attn)))

    def rows_first(x):
        return jnp.transpose(x, (1, 0, 2)).reshape(KEYS, HEADS * HD)

    attn_out = rows_first(results[0])
    d_query, d_key, d_value = rows_first(results[1]), rows_first(results[2]), rows_first(results[3])
    d_pooled = jnp.dot(d_query, w_qkv[0].T, preferred_element_type=jnp.float32)
    d_pooled = d_pooled + jnp.dot(d_key, w_qkv[1].T, preferred_element_type=jnp.float32)
    d_pooled = d_pooled + jnp.dot(d_value, w_qkv[2].T, preferred_element_type=jnp.float32)
    d_pooled = d_pooled.astype(jnp.bfloat16)
    byte_slot = slot[gid]
    byte_grad = (d_pooled[byte_slot].astype(jnp.float32) / lengths[gid][:, None]).astype(jnp.bfloat16)
    return attn_out, byte_grad
```

```python
import functools

import jax
import jax.numpy as jnp
from jax import lax
from jax.experimental import pallas as pl
from jax.experimental.pallas import tpu as pltpu
from jax.sharding import PartitionSpec as P

HD = 128
MESH = pl.DeviceIdType.MESH
VM = pl.BlockSpec(memory_space=pltpu.VMEM)


def remote(src, dst, send, recv, device):
    return pltpu.make_async_remote_copy(
        src_ref=src, dst_ref=dst, send_sem=send, recv_sem=recv, device_id=device, device_id_type=MESH
    )


def whole_kernel(
    n, tp, heads, rows, block,
    bytes_ref, pob_ref, first_ref, moved_ref, w_ref, d_ref,
    attn_ref, grad_ref,
    blk, came, pooled, wbuf, own3, qb, gb, kb, vb, ob, dqb, dkb, dvb, dka, dva,
    o_in, dq_in, dk_in, dv_in, part, own_part, lo_part, hi_part,
    w_sem, send_nb, recv_nb, send_kv, recv_kv, send_qg, recv_qg,
    send_dkv, recv_dkv, send_odq, recv_odq, send_rt, recv_rt, local_sem,
):
    groups = n // heads
    total = n * rows
    half = rows // 2
    scale = HD ** (-0.5)
    bf, f32 = jnp.bfloat16, jnp.float32
    me, mt = lax.axis_index("ctx"), lax.axis_index("tp")
    my_head, my_group = me // groups, lax.rem(me, groups)
    left, right = lax.rem(me + n - 1, n), lax.rem(me + 1, n)
    width = part.shape[2]

    def cols(head):
        return pl.ds(pl.multiple_of(head * HD, HD), HD)

    barrier = pltpu.get_barrier_semaphore()

    def greet(i, carry):
        peer = lax.rem(me + i, n)
        pl.semaphore_signal(barrier, inc=1, device_id=(peer, mt), device_id_type=MESH)
        return carry

    lax.fori_loop(1, n, greet, 0)
    for c in (me, left, right):
        for i in range(1, tp):
            pl.semaphore_signal(
                barrier, inc=1, device_id=(c, lax.rem(mt + i, tp)), device_id_type=MESH
            )
    loads = [pltpu.make_async_copy(w_ref.at[j], wbuf.at[j], w_sem.at[j]) for j in range(3)]
    for j in (1, 2, 0):
        loads[j].start()

    def plan(c):
        below = moved_ref[1, lax.rem(c + n - 1, n)]
        above = moved_ref[0, lax.rem(c + 1, n)]
        start = first_ref[c]
        end = jnp.where(c == n - 1, total, first_ref[lax.rem(c + 1, n)])
        return start, end, below, above, moved_ref[0, c], moved_ref[1, c]

    def numbers(c, rank):
        start, end, below, above, low, high = plan(c)
        return jnp.where(
            rank < below,
            start - below + rank,
            jnp.where(rank >= rows - above, end + rank - (rows - above), start + low + rank - below),
        )

    start, end, below, above, low, high = plan(me)
    count = end - start
    rank = lax.broadcasted_iota(jnp.int32, (2 * rows, 1), 0)
    own_rank = rank - 2 * half
    own_local = jnp.where((own_rank >= below) & (own_rank < rows - above), low + own_rank - below, -1)
    up = jnp.where(rank - half < high, count - high + rank - half, -1)
    wanted = jnp.where(rank < half, rank - half + low, jnp.where(rank < 2 * half, up, own_local))
    pob = pob_ref[...]
    member = (pob == wanted).astype(f32)
    lengths = jnp.maximum(jnp.sum(member, axis=1, keepdims=True), 1.0)
    means = (
        jnp.dot(member.astype(bf), bytes_ref[...], preferred_element_type=f32) / lengths
    ).astype(bf)
    blk[0] = means[:half]
    blk[1] = means[half : 2 * half]
    pl.semaphore_wait(barrier, n - 1 + 3 * (tp - 1))
    near = [
        remote(blk.at[i], came.at[i], send_nb.at[i], recv_nb.at[i], (peer, mt))
        for i, peer in enumerate((left, right))
    ]
    for copy in near:
        copy.start()

    def over_peers(make, wait=False):
        def body(i, carry):
            copy = make(i)
            if wait:
                copy.wait()
            else:
                copy.start()
            return carry

        lax.fori_loop(1, n, body, 0)

    def over_mates(make, wait=False):
        def body(i, carry):
            copy = make(i)
            if wait:
                copy.wait()
            else:
                copy.start()
            return carry

        lax.fori_loop(1, heads, body, 0)

    def to_peer(a, ref, out):
        def make(i):
            peer = lax.rem(me + i, n)
            return remote(
                ref.at[:, cols(peer // groups)], out.at[me], send_kv.at[a, i], recv_kv.at[a, i], (peer, mt)
            )

        return make

    def to_mate(a, ref, out):
        def make(i):
            head = lax.rem(my_head + i, heads)
            return remote(
                ref.at[:, cols(head)], out.at[my_head], send_qg.at[a, i], recv_qg.at[a, i],
                (head * groups + my_group, mt),
            )

        return make

    def back_peer(a, ref, out):
        def make(i):
            peer = lax.rem(me + i, n)
            return remote(
                ref.at[peer], out.at[my_group, :, cols(my_head)], send_dkv.at[a, i], recv_dkv.at[a, i],
                (peer, mt),
            )

        return make

    def back_mate(a, ref, out):
        def make(i):
            head = lax.rem(my_head + i, heads)
            return remote(
                ref.at[head], out.at[:, cols(my_head)], send_odq.at[a, i], recv_odq.at[a, i],
                (head * groups + my_group, mt),
            )

        return make

    mine = cols(my_head)
    send_g = to_mate(0, d_ref, gb)
    send_q = to_mate(1, own3.at[0], qb)
    send_k = to_peer(0, own3.at[1], kb)
    send_v = to_peer(1, own3.at[2], vb)
    over_mates(send_g)
    for copy in near:
        copy.wait()
    pooled[pl.ds(0, half)] = means[2 * half : 3 * half] + came[1]
    pooled[pl.ds(half, half)] = means[3 * half :] + came[0]
    for j, send in ((1, lambda: over_peers(send_k)), (2, lambda: over_peers(send_v)), (0, lambda: over_mates(send_q))):
        loads[j].wait()
        own3[j] = jnp.dot(pooled[...], wbuf[j], preferred_element_type=f32).astype(bf)
        send()
    own = [
        pltpu.make_async_copy(src, dst, local_sem.at[i])
        for i, (src, dst) in enumerate((
            (own3.at[1, :, mine], kb.at[me]), (own3.at[2, :, mine], vb.at[me]),
            (d_ref.at[:, mine], gb.at[my_head]), (own3.at[0, :, mine], qb.at[my_head]),
        ))
    ]
    for copy in own:
        copy.start()
    dka[...] = jnp.zeros_like(dka)
    dva[...] = jnp.zeros_like(dva)
    lane = lax.broadcasted_iota(jnp.int32, (1, total), 1)

    def number_keys(c, ids):
        return jnp.where((lane >= c * rows) & (lane < (c + 1) * rows), numbers(c, lane - c * rows), ids)

    kid = lax.fori_loop(0, n, number_keys, jnp.zeros((1, total), jnp.int32))
    for copy in own:
        copy.wait()
    over_mates(send_g, True)
    over_peers(send_k, True)
    over_peers(send_v, True)
    over_mates(send_q, True)

    over_last = (((1,), (1,)), ((), ()))
    over_first = (((0,), (0,)), ((), ()))
    back_o, back_q = back_mate(0, ob, o_in), back_mate(1, dqb, dq_in)
    row = lax.broadcasted_iota(jnp.int32, (rows, 1), 0)
    step_keys = 128 // rows if rows < 128 else 1
    send_dk, send_dv = back_peer(0, dkb, dk_in), back_peer(1, dvb, dv_in)

    def reach_of(b):
        if b < 0:
            return 0
        reach = min(n, (b + 1) * block * groups + 1)
        return min(n, -(-reach // step_keys) * step_keys)

    for b in reversed(range(heads // block)):
        lo = b * block
        reach, settled = reach_of(b), reach_of(b - 1)
        keys = reach * rows
        q = qb[pl.ds(lo, block)].reshape(block * rows, HD)
        g = gb[pl.ds(lo, block)].reshape(block * rows, HD)
        k = kb[pl.ds(0, reach)].reshape(keys, HD)
        v = vb[pl.ds(0, reach)].reshape(keys, HD)
        qid = jnp.concatenate([numbers((lo + j) * groups + my_group, row) for j in range(block)], axis=0)
        allowed = qid >= kid[:, :keys]
        score = lax.dot_general(q, k, over_last, preferred_element_type=f32) * scale
        score = jnp.where(allowed, score, -jnp.inf)
        top = jnp.max(score, axis=1, keepdims=True)
        e = jnp.exp(score - top)
        prob = e * (1.0 / jnp.sum(e, axis=1, keepdims=True))
        probs = prob.astype(bf)
        out = jnp.dot(probs, v, preferred_element_type=f32).astype(bf)
        delta = jnp.sum(g.astype(f32) * out.astype(f32), axis=1, keepdims=True)
        dprob = lax.dot_general(g, v, over_last, preferred_element_type=f32)
        dscore = (prob * (dprob - delta)).astype(bf)
        dq = (jnp.dot(dscore, k, preferred_element_type=f32) * scale).astype(bf)
        ob[pl.ds(lo, block)] = out.reshape(block, rows, HD)
        dqb[pl.ds(lo, block)] = dq.reshape(block, rows, HD)
        dka[pl.ds(0, keys)] += lax.dot_general(dscore, q, over_first, preferred_element_type=f32)
        dva[pl.ds(0, keys)] += lax.dot_general(probs, g, over_first, preferred_element_type=f32)
        for j in range(block):
            i = lax.rem(lo + j - my_head + heads, heads)

            @pl.when(i != 0)
            def _():
                back_o(i).start()
                back_q(i).start()

        if reach > settled:
            span = pl.ds(settled * rows, (reach - settled) * rows)
            shape = (reach - settled, rows, HD)
            dvb[pl.ds(settled, reach - settled)] = dva[span].astype(bf).reshape(shape)
            dkb[pl.ds(settled, reach - settled)] = (dka[span] * scale).astype(bf).reshape(shape)

            def send_back(peer, carry):
                i = lax.rem(peer - me + n, n)

                @pl.when(i != 0)
                def _():
                    send_dv(i).start()
                    send_dk(i).start()

                return carry

            lax.fori_loop(settled, reach, send_back, 0)

    own = [
        pltpu.make_async_copy(src, dst, local_sem.at[i])
        for i, (src, dst) in enumerate((
            (dkb.at[me], dk_in.at[my_group, :, mine]), (dvb.at[me], dv_in.at[my_group, :, mine]),
            (ob.at[my_head], o_in.at[:, mine]), (dqb.at[my_head], dq_in.at[:, mine]),
        ))
    ]
    for copy in own:
        copy.start()
    for copy in own:
        copy.wait()
    over_mates(back_o, True)
    attn_ref[...] = o_in[...]
    over_mates(back_q, True)
    partial = lax.dot_general(dq_in[...], wbuf[0], over_last, preferred_element_type=f32)
    for send, held, j in ((send_dv, dv_in, 2), (send_dk, dk_in, 1)):
        over_peers(send, True)
        summed = held[0].astype(f32)
        for i in range(1, groups):
            summed = summed + held[i].astype(f32)
        partial += lax.dot_general(summed.astype(bf), wbuf[j], over_last, preferred_element_type=f32)
    for t in range(tp):
        part[t] = partial[:, t * width : (t + 1) * width].astype(bf)
    edge_lo, edge_hi = pl.ds(0, half), pl.ds(rows - half, half)
    copies = []
    for i in range(1, tp):
        t = lax.rem(mt + i, tp)
        copies.append((part.at[t], own_part.at[mt], (me, t)))
    for i in range(tp):
        t = lax.rem(mt + i, tp)
        copies.append((part.at[t, edge_lo], hi_part.at[mt], (left, t)))
        copies.append((part.at[t, edge_hi], lo_part.at[mt], (right, t)))
    copies = [
        remote(src, dst, send_rt.at[i], recv_rt.at[i], peer) for i, (src, dst, peer) in enumerate(copies)
    ]
    for copy in copies:
        copy.start()
    kept = pltpu.make_async_copy(part.at[mt], own_part.at[mt], local_sem.at[0])
    kept.start()
    target = jnp.where(
        pob < low,
        half - low + pob,
        jnp.where(pob >= count - high, half + rows + pob - (count - high), half + below + pob - low),
    )
    chooser = (target == lax.broadcasted_iota(jnp.int32, (2 * rows, 1), 0)).astype(f32)
    sizes = jnp.maximum(jnp.sum(chooser, axis=1, keepdims=True), 1.0)
    kept.wait()
    for copy in copies:
        copy.wait()

    def over_tp(ref):
        value = ref[0].astype(f32)
        for i in range(1, tp):
            value = value + ref[i].astype(f32)
        return value

    returned = jnp.concatenate([over_tp(lo_part), over_tp(own_part), over_tp(hi_part)], axis=0)
    shares = (returned.astype(bf).astype(f32) / sizes).astype(bf)
    grad_ref[...] = lax.dot_general(
        chooser.astype(bf), shares, over_first, preferred_element_type=f32
    ).astype(bf)


def emit_kernel(a_ref, g_ref, a_out, g_out, sem):
    copies = [
        pltpu.make_async_copy(src, dst, sem.at[i]) for i, (src, dst) in enumerate(((a_ref, a_out), (g_ref, g_out)))
    ]
    for copy in copies:
        copy.start()
    for copy in copies:
        copy.wait()


def shards(byte_states, patch_of_byte, patch_first, moved, w_qkv, d_attn):
    n, tp = lax.axis_size("ctx"), lax.axis_size("tp")
    rows, feats = d_attn.shape
    size, model = byte_states.shape
    heads = feats // HD
    groups = n // heads
    total = n * rows
    half = rows // 2
    width = model // tp
    block = 2 if heads % 2 == 0 else 1
    bf, f32 = jnp.bfloat16, jnp.float32
    dma = pltpu.SemaphoreType.DMA
    smem = pl.BlockSpec(memory_space=pltpu.SMEM)
    results = pl.pallas_call(
        functools.partial(whole_kernel, n, tp, heads, rows, block),
        out_shape=[pltpu.VMEM((rows, feats), bf), pltpu.VMEM((size, width), bf)],
        in_specs=[VM, VM, smem, smem, pl.BlockSpec(memory_space=pl.ANY), VM],
        out_specs=[VM] * 2,
        scratch_shapes=[
            pltpu.VMEM((2, half, model), bf), pltpu.VMEM((2, half, model), bf),
            pltpu.VMEM((rows, model), bf), pltpu.VMEM(w_qkv.shape, bf), pltpu.VMEM((3, rows, feats), bf),
            pltpu.VMEM((heads, rows, HD), bf), pltpu.VMEM((heads, rows, HD), bf),
            pltpu.VMEM((n, rows, HD), bf), pltpu.VMEM((n, rows, HD), bf),
            pltpu.VMEM((heads, rows, HD), bf), pltpu.VMEM((heads, rows, HD), bf),
            pltpu.VMEM((n, rows, HD), bf), pltpu.VMEM((n, rows, HD), bf),
            pltpu.VMEM((total, HD), f32), pltpu.VMEM((total, HD), f32),
            pltpu.VMEM((rows, feats), bf), pltpu.VMEM((rows, feats), bf),
            pltpu.VMEM((groups, rows, feats), bf), pltpu.VMEM((groups, rows, feats), bf),
            pltpu.VMEM((tp, rows, width), bf), pltpu.VMEM((tp, rows, width), bf),
            pltpu.VMEM((tp, half, width), bf), pltpu.VMEM((tp, half, width), bf),
            dma((3,)), dma((2,)), dma((2,)), dma((2, n)), dma((2, n)), dma((2, heads)), dma((2, heads)),
            dma((2, n)), dma((2, n)), dma((2, heads)), dma((2, heads)),
            dma((3 * tp - 1,)), dma((3 * tp - 1,)), dma((4,)),
        ],
        compiler_params=pltpu.CompilerParams(
            collective_id=0, has_side_effects=True, vmem_limit_bytes=60 << 20
        ),
        name="whole",
    )(byte_states, patch_of_byte.reshape(1, size), patch_first, moved, w_qkv, d_attn)
    results = [pltpu.with_memory_space_constraint(x, pltpu.VMEM) for x in results]
    return tuple(pl.pallas_call(
        emit_kernel,
        out_shape=[jax.ShapeDtypeStruct((rows, feats), bf), jax.ShapeDtypeStruct((size, width), bf)],
        in_specs=[VM, VM],
        out_specs=[pl.BlockSpec(memory_space=pl.ANY)] * 2,
        scratch_shapes=[dma((2,))],
        name="emit",
    )(*results))


def solution(mesh):
    placed = (P("ctx", None), P("ctx"), P(), P(), P(None, None, "tp"), P("ctx", "tp"))
    return jax.shard_map(
        shards,
        mesh=mesh,
        in_specs=placed,
        out_specs=(P("ctx", "tp"), P("ctx", "tp")),
        check_vma=False,
    )
```

```python
import functools

import jax
import jax.numpy as jnp
from jax import lax
from jax.experimental import pallas as pl
from jax.experimental.pallas import tpu as pltpu
from jax.sharding import PartitionSpec as P

HD = 128
MESH = pl.DeviceIdType.MESH
VM = pl.BlockSpec(memory_space=pltpu.VMEM)
ANY = pl.BlockSpec(memory_space=pl.ANY)


def remote(src, dst, send, recv, device):
    return pltpu.make_async_remote_copy(
        src_ref=src, dst_ref=dst, send_sem=send, recv_sem=recv, device_id=device, device_id_type=MESH
    )


def each(lo, hi, act):
    def body(i, carry):
        act(i)
        return carry

    lax.fori_loop(lo, hi, body, 0)


def whole_kernel(
    n, tp, heads, rows, block, per,
    bytes_hbm, pob_hbm, first_hbm, moved_hbm, w_hbm, d_hbm,
    attn_ref, grad_ref,
    bytes_ref, pob_ref, first_ref, moved_ref, wbuf, d_ref,
    blk, came, pooled, own3, qb, gb, kb, vb, ob, dqb, dkb, dvb, xk, xv, dka, dva,
    o_in, dq_in, dk_in, dv_in, part, own_part, lo_part, hi_part,
    in_sem, w_sem, send_nb, recv_nb, send_kv, recv_kv, send_fw, recv_fw, send_qg, recv_qg,
    send_mg, recv_mg, send_dkv, recv_dkv, send_odq, recv_odq, send_rt, recv_rt, local_sem,
):
    pairs = n // 2
    groups = pairs // heads
    stride = 2 * groups
    total = n * rows
    half = rows // 2
    scale = HD ** (-0.5)
    bf, f32 = jnp.bfloat16, jnp.float32
    me, mt = lax.axis_index("ctx"), lax.axis_index("tp")
    sub = lax.rem(mt, 2)
    base = mt - sub
    mate = (me, base + 1 - sub)
    parity, place = lax.rem(me, 2), me // 2
    source_tp = base + parity
    my_head, my_group = place // groups, lax.rem(place, groups)
    offset = 2 * my_group + sub
    slot = me // stride
    left, right = lax.rem(me + n - 1, n), lax.rem(me + 1, n)
    has_left, has_right = me > 0, me < n - 1
    width = part.shape[2]

    def cols(head, count=1):
        return pl.ds(pl.multiple_of(head * HD, HD), count * HD)

    barrier = pltpu.get_barrier_semaphore()

    def greet(i):
        peer = lax.rem(me + i, n)
        for core in range(2):
            pl.semaphore_signal(barrier, inc=1, device_id=(peer, base + core), device_id_type=MESH)

    pl.semaphore_signal(barrier, inc=1, device_id=mate, device_id_type=MESH)
    each(1, n, greet)
    for c in (me, left, right):
        for i in range(2, tp):
            pl.semaphore_signal(
                barrier, inc=1, device_id=(c, lax.rem(base + i, tp)), device_id_type=MESH
            )
    inputs = [
        pltpu.make_async_copy(src, dst, in_sem.at[i])
        for i, (src, dst) in enumerate((
            (pob_hbm, pob_ref), (first_hbm, first_ref), (moved_hbm, moved_ref), (bytes_hbm, bytes_ref),
            (d_hbm, d_ref),
        ))
    ]
    for copy in inputs:
        copy.start()
    loads = [pltpu.make_async_copy(w_hbm.at[j], wbuf.at[j], w_sem.at[j]) for j in range(3)]
    for copy in inputs[:3]:
        copy.wait()

    def plan(c):
        below = moved_ref[1, lax.rem(c + n - 1, n)]
        above = moved_ref[0, lax.rem(c + 1, n)]
        start = first_ref[c]
        end = jnp.where(c == n - 1, total, first_ref[lax.rem(c + 1, n)])
        return start, end, below, above, moved_ref[0, c], moved_ref[1, c]

    def numbers(c, rank):
        start, end, below, above, low, high = plan(c)
        return jnp.where(
            rank < below,
            start - below + rank,
            jnp.where(rank >= rows - above, end + rank - (rows - above), start + low + rank - below),
        )

    start, end, below, above, low, high = plan(me)
    count = end - start
    rank = lax.broadcasted_iota(jnp.int32, (2 * rows, 1), 0)
    own_rank = rank - 2 * half
    own_local = jnp.where((own_rank >= below) & (own_rank < rows - above), low + own_rank - below, -1)
    up = jnp.where(rank - half < high, count - high + rank - half, -1)
    wanted = jnp.where(rank < half, rank - half + low, jnp.where(rank < 2 * half, up, own_local))
    pob = pob_ref[...]
    member = (pob == wanted).astype(f32)
    lengths = jnp.maximum(jnp.sum(member, axis=1, keepdims=True), 1.0)
    inputs[3].wait()
    for j in (1, 0, 2):
        loads[j].start()
    means = (
        jnp.dot(member.astype(bf), bytes_ref[...], preferred_element_type=f32) / lengths
    ).astype(bf)
    blk[0] = means[:half]
    blk[1] = means[half : 2 * half]

    @pl.when(me == 0)
    def _():
        came[1] = jnp.zeros_like(came[1])
        lo_part[...] = jnp.zeros_like(lo_part)

    @pl.when(me == n - 1)
    def _():
        came[0] = jnp.zeros_like(came[0])
        hi_part[...] = jnp.zeros_like(hi_part)

    pl.semaphore_wait(barrier, 2 * n - 1 + 3 * (tp - 2))
    to_left = remote(blk.at[0], came.at[0], send_nb.at[0], recv_nb.at[0], (left, mt))
    to_right = remote(blk.at[1], came.at[1], send_nb.at[1], recv_nb.at[1], (right, mt))
    pl.when(has_left)(to_left.start)
    pl.when(has_right)(to_right.start)

    def send_block(a, ref, out):
        def make(i):
            chip = 2 * i + sub
            return chip, remote(
                ref.at[:, cols(i // groups)], out.at[me], send_kv.at[a, i], recv_kv.at[a, place],
                (chip, base + parity),
            )

        return make

    def send_query(a, ref, out):
        def make(h):
            chip = 2 * (h * groups + my_group) + sub
            return chip, remote(
                ref.at[:, cols(h)], out.at[slot], send_qg.at[a, h], recv_qg.at[a, slot],
                (chip, base + parity),
            )

        return make

    def forward(a, ref, block_at):
        return remote(
            ref.at[block_at], ref.at[block_at], send_fw.at[a, block_at // 2], recv_fw.at[a, block_at // 2], mate
        )

    def back_query(a, ref, out):
        def make(j):
            c = j * stride + offset
            return c, remote(
                ref.at[j], out.at[:, cols(my_head)], send_odq.at[a, j], recv_odq.at[a, my_head], (c, source_tp)
            )

        return make

    def back_block(a, ref, out):
        def make(i):
            c = 2 * i + sub
            return c, remote(
                ref.at[c], out.at[my_group, :, cols(my_head)], send_dkv.at[a, i], recv_dkv.at[a, place],
                (c, source_tp),
            )

        return make

    def start_each(lo, hi, make):
        def act(i):
            other, copy = make(i)
            pl.when(other != me)(copy.start)

        each(lo, hi, act)

    def sent_each(lo, hi, make):
        def act(i):
            other, copy = make(i)
            pl.when(other != me)(copy.wait_send)

        each(lo, hi, act)

    send_g, send_q = send_query(0, d_ref, gb), send_query(1, own3.at[0], qb)
    send_k, send_v = send_block(0, own3.at[1], kb), send_block(1, own3.at[2], vb)
    inputs[4].wait()
    start_each(0, heads, send_g)
    lane = lax.broadcasted_iota(jnp.int32, (1, total), 1)

    def number_keys(c, ids):
        return jnp.where((lane >= c * rows) & (lane < (c + 1) * rows), numbers(c, lane - c * rows), ids)

    kid = lax.fori_loop(0, n, number_keys, jnp.zeros((1, total), jnp.int32))
    dka[...] = jnp.zeros_like(dka)
    dva[...] = jnp.zeros_like(dva)
    pl.when(has_left)(to_right.wait_recv)
    pl.when(has_right)(to_left.wait_recv)
    pooled[pl.ds(0, half)] = means[2 * half : 3 * half] + came[1]
    pooled[pl.ds(half, half)] = means[3 * half :] + came[0]
    chunks = heads // per
    mine = cols(my_head)
    for j, make in ((1, send_k), (0, send_q), (2, send_v)):
        loads[j].wait()
        for s in range(chunks):
            chunk = lax.rem(my_head // per + (chunks + 1) // 2 + s, chunks)
            span = cols(chunk * per, per)
            own3[j, :, span] = jnp.dot(
                pooled[...], wbuf[j, :, span], preferred_element_type=f32
            ).astype(bf)
            each_head = per if j == 0 else per * groups
            start_each(chunk * each_head, (chunk + 1) * each_head, make)

    @pl.when(parity == sub)
    def _():
        qb[slot] = own3[0, :, mine]
        kb[me] = own3[1, :, mine]
        vb[me] = own3[2, :, mine]
        gb[slot] = d_ref[:, mine]

    def take_blocks(a, ref):
        def act(i):
            c = 2 * i + sub
            pl.when(c != me)(remote(
                ref.at[c], ref.at[c], send_kv.at[a, i], recv_kv.at[a, i], (c, source_tp)
            ).wait_recv)
            forward(a, ref, c).start()

        each(0, pairs, act)

    def take_forwards(a, ref):
        each(0, pairs, lambda i: forward(a, ref, 2 * i + 1 - sub).wait_recv())

    def take_queries(a, ref):
        def act(j):
            c = j * stride + offset
            pl.when(c != me)(remote(
                ref.at[j], ref.at[j], send_qg.at[a, j], recv_qg.at[a, j], (c, source_tp)
            ).wait_recv)

        each(0, heads, act)

    take_blocks(0, kb)
    take_queries(1, qb)
    take_forwards(0, kb)
    take_blocks(1, vb)
    take_forwards(1, vb)
    take_queries(0, gb)

    over_last = (((1,), (1,)), ((), ()))
    over_first = (((0,), (0,)), ((), ()))
    back_o, back_q = back_query(0, ob, o_in), back_query(1, dqb, dq_in)
    back_k, back_v = back_block(0, dkb, dk_in), back_block(1, dvb, dv_in)
    row = lax.broadcasted_iota(jnp.int32, (rows, 1), 0)
    step_keys = max(2, 128 // rows)

    def reach_of(b):
        if b < 0:
            return 0
        reach = min(n, (b + 1) * block * stride + 1)
        return min(n, -(-reach // step_keys) * step_keys)

    def at(c):
        return pl.ds(pl.multiple_of(c * rows, rows), rows)

    def hand_over(lo, hi):
        def act(i):
            c = 2 * i + 1 - sub
            for a, (acc, buf, out, factor) in enumerate(((dka, dkb, xk, scale), (dva, dvb, xv, None))):
                value = acc[at(c)]
                buf[c] = (value if factor is None else value * factor).astype(bf)
                remote(buf.at[c], out.at[i], send_mg.at[a, i], recv_mg.at[a, i], mate).start()

        each(lo // 2, hi // 2, act)

    def send_home(lo, hi):
        def act(i):
            c = 2 * i + sub
            for a, (acc, buf, got, factor, make) in enumerate((
                (dka, dkb, xk, scale, back_k), (dva, dvb, xv, None, back_v)
            )):
                remote(buf.at[c], got.at[i], send_mg.at[a, i], recv_mg.at[a, i], mate).wait_recv()
                value = acc[at(c)]
                value = value if factor is None else value * factor
                buf[c] = (value + got[i].astype(f32)).astype(bf)
                pl.when(c != me)(make(i)[1].start)

        each(lo // 2, hi // 2, act)

    late = None
    for b in reversed(range(heads // block)):
        lo = b * block
        reach, settled = reach_of(b), reach_of(b - 1)
        keys = reach * rows
        q = qb[pl.ds(lo, block)].reshape(block * rows, HD)
        g = gb[pl.ds(lo, block)].reshape(block * rows, HD)
        k = kb[pl.ds(0, reach)].reshape(keys, HD)
        v = vb[pl.ds(0, reach)].reshape(keys, HD)
        qid = jnp.concatenate([numbers((lo + j) * stride + offset, row) for j in range(block)], axis=0)
        allowed = qid >= kid[:, :keys]
        score = lax.dot_general(q, k, over_last, preferred_element_type=f32) * scale
        score = jnp.where(allowed, score, -jnp.inf)
        top = jnp.max(score, axis=1, keepdims=True)
        e = jnp.exp(score - top)
        prob = e * (1.0 / jnp.sum(e, axis=1, keepdims=True))
        probs = prob.astype(bf)
        out = jnp.dot(probs, v, preferred_element_type=f32).astype(bf)
        delta = jnp.sum(g.astype(f32) * out.astype(f32), axis=1, keepdims=True)
        dprob = lax.dot_general(g, v, over_last, preferred_element_type=f32)
        dscore = (prob * (dprob - delta)).astype(bf)
        dq = (jnp.dot(dscore, k, preferred_element_type=f32) * scale).astype(bf)
        ob[pl.ds(lo, block)] = out.reshape(block, rows, HD)
        dqb[pl.ds(lo, block)] = dq.reshape(block, rows, HD)
        dka[pl.ds(0, keys)] += lax.dot_general(dscore, q, over_first, preferred_element_type=f32)
        dva[pl.ds(0, keys)] += lax.dot_general(probs, g, over_first, preferred_element_type=f32)
        start_each(lo, lo + block, back_o)
        start_each(lo, lo + block, back_q)
        if reach > settled:
            hand_over(settled, reach)
        if late is not None:
            send_home(*late)
        late = (settled, reach) if reach > settled else None
    if late is not None:
        send_home(*late)

    @pl.when(parity == sub)
    def _():
        o_in[:, mine] = ob[slot]
        dq_in[:, mine] = dqb[slot]
        dk_in[my_group, :, mine] = dkb[me]
        dv_in[my_group, :, mine] = dvb[me]

    def take_back(a, into):
        def act(h):
            chip = 2 * (h * groups + my_group) + sub
            pl.when(chip != me)(remote(
                into.at[:, cols(h)], into.at[:, cols(h)], send_odq.at[a, h], recv_odq.at[a, h],
                (chip, base + parity),
            ).wait_recv)

        each(0, heads, act)

    def take_back_blocks(a, into):
        def act(i):
            chip = 2 * i + sub
            there = into.at[lax.rem(i, groups), :, cols(i // groups)]
            pl.when(chip != me)(remote(
                there, there, send_dkv.at[a, i], recv_dkv.at[a, i], (chip, base + parity)
            ).wait_recv)

        each(0, pairs, act)

    take_back(0, o_in)
    attn_ref[...] = o_in[...]
    take_back(1, dq_in)
    partial = lax.dot_general(dq_in[...], wbuf[0], over_last, preferred_element_type=f32)
    for a, held, j in ((1, dv_in, 2), (0, dk_in, 1)):
        take_back_blocks(a, held)
        summed = held[0]
        if groups > 1:
            summed = summed.astype(f32)
            for i in range(1, groups):
                summed = summed + held[i].astype(f32)
            summed = summed.astype(bf)
        partial += lax.dot_general(summed, wbuf[j], over_last, preferred_element_type=f32)
    for t in range(tp):
        part[t] = partial[:, t * width : (t + 1) * width].astype(bf)
    edge_lo, edge_hi = pl.ds(0, half), pl.ds(rows - half, half)
    copies = []
    for i in range(tp):
        t = lax.rem(mt + i, tp)
        copies.append((has_left, has_right, remote(
            part.at[t, edge_lo], hi_part.at[mt], send_rt.at[0, i], recv_rt.at[0, i], (left, t)
        )))
        copies.append((has_right, has_left, remote(
            part.at[t, edge_hi], lo_part.at[mt], send_rt.at[1, i], recv_rt.at[1, i], (right, t)
        )))
        if i > 0:
            copies.append((None, None, remote(
                part.at[t], own_part.at[mt], send_rt.at[2, i], recv_rt.at[2, i], (me, t)
            )))
    for sends, _, copy in copies:
        copy.start() if sends is None else pl.when(sends)(copy.start)
    own_part[mt] = part[mt]
    target = jnp.where(
        pob < low,
        half - low + pob,
        jnp.where(pob >= count - high, half + rows + pob - (count - high), half + below + pob - low),
    )
    chooser = (target == lax.broadcasted_iota(jnp.int32, (2 * rows, 1), 0)).astype(f32)
    sizes = jnp.maximum(jnp.sum(chooser, axis=1, keepdims=True), 1.0)
    pl.when(has_left)(to_left.wait_send)
    pl.when(has_right)(to_right.wait_send)
    sent_each(0, heads, send_g)
    sent_each(0, heads, send_q)
    sent_each(0, pairs, send_k)
    sent_each(0, pairs, send_v)
    sent_each(0, heads, back_o)
    sent_each(0, heads, back_q)
    sent_each(0, pairs, back_k)
    sent_each(0, pairs, back_v)

    def sent_to_mate(i):
        for a, (ref, acc, got) in enumerate(((kb, dkb, xk), (vb, dvb, xv))):
            forward(a, ref, 2 * i + sub).wait_send()
            remote(acc.at[2 * i], got.at[i], send_mg.at[a, i], recv_mg.at[a, i], mate).wait_send()

    each(0, pairs, sent_to_mate)
    for sends, comes, copy in copies:
        copy.wait_recv() if comes is None else pl.when(comes)(copy.wait_recv)
        copy.wait_send() if sends is None else pl.when(sends)(copy.wait_send)

    def over_tp(ref):
        value = ref[0].astype(f32)
        for i in range(1, tp):
            value = value + ref[i].astype(f32)
        return value

    returned = jnp.concatenate([over_tp(lo_part), over_tp(own_part), over_tp(hi_part)], axis=0)
    shares = (returned.astype(bf).astype(f32) / sizes).astype(bf)
    grad_ref[...] = lax.dot_general(
        chooser.astype(bf), shares, over_first, preferred_element_type=f32
    ).astype(bf)


def emit_kernel(a_ref, g_ref, a_out, g_out, sem):
    copies = [
        pltpu.make_async_copy(src, dst, sem.at[i]) for i, (src, dst) in enumerate(((a_ref, a_out), (g_ref, g_out)))
    ]
    for copy in copies:
        copy.start()
    for copy in copies:
        copy.wait()


def shards(byte_states, patch_of_byte, patch_first, moved, w_qkv, d_attn):
    n, tp = lax.axis_size("ctx"), lax.axis_size("tp")
    rows, feats = d_attn.shape
    size, model = byte_states.shape
    heads = feats // HD
    pairs = n // 2
    groups = pairs // heads
    total = n * rows
    half = rows // 2
    width = model // tp
    block = per = 2 if heads % 2 == 0 else 1
    assert tp % 2 == 0 and n % 2 == 0 and pairs % heads == 0
    bf, f32, i32 = jnp.bfloat16, jnp.float32, jnp.int32
    dma = pltpu.SemaphoreType.DMA
    results = pl.pallas_call(
        functools.partial(whole_kernel, n, tp, heads, rows, block, per),
        out_shape=[pltpu.VMEM((rows, feats), bf), pltpu.VMEM((size, width), bf)],
        in_specs=[ANY] * 6,
        out_specs=[VM] * 2,
        scratch_shapes=[
            pltpu.VMEM((size, model), bf), pltpu.VMEM((1, size), i32),
            pltpu.SMEM((n,), i32), pltpu.SMEM((2, n), i32),
            pltpu.VMEM(w_qkv.shape, bf), pltpu.VMEM((rows, feats), bf),
            pltpu.VMEM((2, half, model), bf), pltpu.VMEM((2, half, model), bf),
            pltpu.VMEM((rows, model), bf), pltpu.VMEM((3, rows, feats), bf),
            pltpu.VMEM((heads, rows, HD), bf), pltpu.VMEM((heads, rows, HD), bf),
            pltpu.VMEM((n, rows, HD), bf), pltpu.VMEM((n, rows, HD), bf),
            pltpu.VMEM((heads, rows, HD), bf), pltpu.VMEM((heads, rows, HD), bf),
            pltpu.VMEM((n, rows, HD), bf), pltpu.VMEM((n, rows, HD), bf),
            pltpu.VMEM((pairs, rows, HD), bf), pltpu.VMEM((pairs, rows, HD), bf),
            pltpu.VMEM((total, HD), f32), pltpu.VMEM((total, HD), f32),
            pltpu.VMEM((rows, feats), bf), pltpu.VMEM((rows, feats), bf),
            pltpu.VMEM((groups, rows, feats), bf), pltpu.VMEM((groups, rows, feats), bf),
            pltpu.VMEM((tp, rows, width), bf), pltpu.VMEM((tp, rows, width), bf),
            pltpu.VMEM((tp, half, width), bf), pltpu.VMEM((tp, half, width), bf),
            dma((5,)), dma((3,)), dma((2,)), dma((2,)), dma((2, pairs)), dma((2, pairs)),
            dma((2, pairs)), dma((2, pairs)), dma((2, heads)), dma((2, heads)),
            dma((2, pairs)), dma((2, pairs)), dma((2, pairs)), dma((2, pairs)),
            dma((2, heads)), dma((2, heads)), dma((3, tp)), dma((3, tp)), dma((4,)),
        ],
        compiler_params=pltpu.CompilerParams(
            collective_id=0, has_side_effects=True, vmem_limit_bytes=60 << 20
        ),
        name="whole",
    )(byte_states, patch_of_byte.reshape(1, size), patch_first, moved, w_qkv, d_attn)
    results = [pltpu.with_memory_space_constraint(x, pltpu.VMEM) for x in results]
    return tuple(pl.pallas_call(
        emit_kernel,
        out_shape=[jax.ShapeDtypeStruct((rows, feats), bf), jax.ShapeDtypeStruct((size, width), bf)],
        in_specs=[VM, VM],
        out_specs=[ANY] * 2,
        scratch_shapes=[dma((2,))],
        name="emit",
    )(*results))


def solution(mesh):
    placed = (P("ctx", None), P("ctx"), P(), P(), P(None, None, "tp"), P("ctx", "tp"))
    return jax.shard_map(
        shards,
        mesh=mesh,
        in_specs=placed,
        out_specs=(P("ctx", "tp"), P("ctx", "tp")),
        check_vma=False,
    )
```

```python
import functools

import jax
import jax.numpy as jnp
from jax import lax
from jax.experimental import pallas as pl
from jax.experimental.pallas import tpu as pltpu
from jax.sharding import PartitionSpec as P

HD = 128
MESH = pl.DeviceIdType.MESH
VM = pl.BlockSpec(memory_space=pltpu.VMEM)
ANY = pl.BlockSpec(memory_space=pl.ANY)


def remote(src, dst, send, recv, device):
    return pltpu.make_async_remote_copy(
        src_ref=src, dst_ref=dst, send_sem=send, recv_sem=recv, device_id=device, device_id_type=MESH
    )


def each(lo, hi, act):
    def body(i, carry):
        act(i)
        return carry

    lax.fori_loop(lo, hi, body, 0)


def whole_kernel(
    n, tp, heads, rows, block, per,
    bytes_hbm, pob_hbm, first_hbm, moved_hbm, w_hbm, d_hbm,
    attn_ref, grad_ref,
    bytes_ref, pob_ref, first_ref, moved_ref, wbuf, d_ref,
    blk, came, pooled, own3, qb, gb, kb, vb, pa, ob, dqb, dkv, xkv, dka, dva,
    o_in, dq_in, dkv_in, part, own_part, lo_part, hi_part, tally,
    in_sem, w_sem, send_nb, recv_nb, send_x, recv_x, send_f, recv_f, send_m, recv_m,
    send_h, recv_o, recv_b, send_r, recv_r,
):
    pairs = n // 2
    groups = pairs // heads
    stride = 2 * groups
    total = n * rows
    half = rows // 2
    scale = HD ** (-0.5)
    bf, f32 = jnp.bfloat16, jnp.float32
    me, mt = lax.axis_index("ctx"), lax.axis_index("tp")
    sub = lax.rem(mt, 2)
    base = mt - sub
    mate = (me, base + 1 - sub)
    parity, place = lax.rem(me, 2), me // 2
    source_tp = base + parity
    at_home = parity == sub
    my_head, my_group = place // groups, lax.rem(place, groups)
    offset = 2 * my_group + sub
    slot = me // stride
    left, right = lax.rem(me + n - 1, n), lax.rem(me + 1, n)
    has_left, has_right = me > 0, me < n - 1
    width = part.shape[2]

    def cols(head, count=1):
        return pl.ds(pl.multiple_of(head * HD, HD), count * HD)

    chunks = heads // per

    def order(s):
        if chunks % 2:
            return lax.rem(my_head // per + (chunks + 1) // 2 + s, chunks)
        here, mid = my_head // per, chunks // 2
        upper = here // mid
        if s < mid:
            return (1 - upper) * (chunks - 1 - s) + upper * s
        back = chunks - 1 - s
        return upper * mid + lax.rem(here + back, mid)

    barrier = pltpu.get_barrier_semaphore()

    def greet(i):
        peer = lax.rem(me + i, n)
        for core in range(2):
            pl.semaphore_signal(barrier, inc=1, device_id=(peer, base + core), device_id_type=MESH)

    pl.semaphore_signal(barrier, inc=1, device_id=mate, device_id_type=MESH)
    each(1, n, greet)
    for c in (me, left, right):
        for i in range(2, tp):
            pl.semaphore_signal(
                barrier, inc=1, device_id=(c, lax.rem(base + i, tp)), device_id_type=MESH
            )
    inputs = [
        pltpu.make_async_copy(src, dst, in_sem.at[i])
        for i, (src, dst) in enumerate((
            (pob_hbm, pob_ref), (first_hbm, first_ref), (moved_hbm, moved_ref), (bytes_hbm, bytes_ref),
            (d_hbm, d_ref),
        ))
    ]
    for copy in inputs:
        copy.start()
    loads = [pltpu.make_async_copy(w_hbm.at[j], wbuf.at[j], w_sem.at[j]) for j in range(3)]
    for copy in inputs[:3]:
        copy.wait()

    def plan(c):
        below = moved_ref[1, lax.rem(c + n - 1, n)]
        above = moved_ref[0, lax.rem(c + 1, n)]
        start = first_ref[c]
        end = jnp.where(c == n - 1, total, first_ref[lax.rem(c + 1, n)])
        return start, end, below, above, moved_ref[0, c], moved_ref[1, c]

    def numbers(c, rank):
        start, end, below, above, low, high = plan(c)
        return jnp.where(
            rank < below,
            start - below + rank,
            jnp.where(rank >= rows - above, end + rank - (rows - above), start + low + rank - below),
        )

    start, end, below, above, low, high = plan(me)
    count = end - start
    rank = lax.broadcasted_iota(jnp.int32, (2 * rows, 1), 0)
    own_rank = rank - 2 * half
    own_local = jnp.where((own_rank >= below) & (own_rank < rows - above), low + own_rank - below, -1)
    up = jnp.where(rank - half < high, count - high + rank - half, -1)
    wanted = jnp.where(rank < half, rank - half + low, jnp.where(rank < 2 * half, up, own_local))
    pob = pob_ref[...]
    member = (pob == wanted).astype(f32)
    lengths = jnp.maximum(jnp.sum(member, axis=1, keepdims=True), 1.0)
    inputs[3].wait()
    for j in (1, 0, 2):
        loads[j].start()
    means = (
        jnp.dot(member.astype(bf), bytes_ref[...], preferred_element_type=f32) / lengths
    ).astype(bf)
    blk[0] = means[:half]
    blk[1] = means[half : 2 * half]

    @pl.when(me == 0)
    def _():
        came[1] = jnp.zeros_like(came[1])
        lo_part[...] = jnp.zeros_like(lo_part)

    @pl.when(me == n - 1)
    def _():
        came[0] = jnp.zeros_like(came[0])
        hi_part[...] = jnp.zeros_like(hi_part)

    pl.semaphore_wait(barrier, 2 * n - 1 + 3 * (tp - 2))
    to_left = remote(blk.at[0], came.at[0], send_nb.at[0], recv_nb.at[0], (left, mt))
    to_right = remote(blk.at[1], came.at[1], send_nb.at[1], recv_nb.at[1], (right, mt))
    pl.when(has_left)(to_left.start)
    pl.when(has_right)(to_right.start)

    def amount(count):
        return tally.at[pl.ds(0, count)]

    def came_in(sem, count):
        remote(amount(count), amount(count), sem, sem, mate).wait_recv()

    def went_out(sem, count):
        remote(amount(count), amount(count), sem, sem, mate).wait_send()

    def but_own(wait, sem, count, own=1):
        pl.when(at_home)(lambda: wait(sem, count - own))
        pl.when(jnp.logical_not(at_home))(lambda: wait(sem, count))

    def start_each(lo, hi, make):
        def act(i):
            other, copy = make(i)
            pl.when(other != me)(copy.start)

        each(lo, hi, act)

    def send_block(a, ref, out):
        def make(i):
            chip = 2 * i + sub
            return chip, remote(
                ref.at[:, cols(i // groups)], out.at[place, parity], send_x.at[a], recv_x.at[a],
                (chip, base + parity),
            )

        return make

    def send_query(a, ref, out):
        def make(h):
            chip = 2 * (h * groups + my_group) + sub
            return chip, remote(
                ref.at[:, cols(h)], out.at[slot], send_x.at[a], recv_x.at[a], (chip, base + parity)
            )

        return make

    def forward(a, ref):
        return remote(ref.at[:, sub], ref.at[:, sub], send_f.at[a], recv_f.at[a], mate)

    def back_query(a, ref, out):
        def make(j):
            c = j * stride + offset
            return c, remote(
                ref.at[j], out.at[:, cols(my_head)], send_h.at[a], recv_o.at[0] if a == 0 else recv_b.at[my_head // per],
                (c, source_tp),
            )

        return make

    def back_block(a):
        def make(i):
            c = 2 * i + sub
            return c, remote(
                dkv.at[a, i, sub], dkv_in.at[a, my_group, :, cols(my_head)], send_h.at[2 + a],
                recv_b.at[my_head // per], (c, source_tp),
            )

        return make

    send_g, send_q = send_query(3, d_ref, gb), send_query(2, own3.at[0], qb)
    send_k, send_v = send_block(0, own3.at[1], kb), send_block(1, own3.at[2], vb)
    lane = lax.broadcasted_iota(jnp.int32, (1, total), 1)

    def number_keys(c, ids):
        return jnp.where((lane >= c * rows) & (lane < (c + 1) * rows), numbers(c, lane - c * rows), ids)

    kid = lax.fori_loop(0, n, number_keys, jnp.zeros((1, total), jnp.int32))
    dka[...] = jnp.zeros_like(dka)
    dva[...] = jnp.zeros_like(dva)
    pl.when(has_left)(to_right.wait_recv)
    pl.when(has_right)(to_left.wait_recv)
    pooled[pl.ds(0, half)] = means[2 * half : 3 * half] + came[1]
    pooled[pl.ds(half, half)] = means[3 * half :] + came[0]
    mine = cols(my_head)
    for j, make in ((1, send_k), (0, send_q), (2, send_v)):
        loads[j].wait()
        for s in range(chunks):
            chunk = order(s)
            span = cols(chunk * per, per)
            own3[j, :, span] = jnp.dot(
                pooled[...], wbuf[j, :, span], preferred_element_type=f32
            ).astype(bf)
            each_head = per if j == 0 else per * groups
            start_each(chunk * each_head, (chunk + 1) * each_head, make)
    inputs[4].wait()
    start_each(0, heads, send_g)

    @pl.when(parity == sub)
    def _():
        qb[slot] = own3[0, :, mine]
        kb[place, parity] = own3[1, :, mine]
        vb[place, parity] = own3[2, :, mine]
        gb[slot] = d_ref[:, mine]

    over_last = (((1,), (1,)), ((), ()))
    over_first = (((0,), (0,)), ((), ()))
    back_o, back_q = back_query(0, ob, o_in), back_query(1, dqb, dq_in)
    back_k, back_v = back_block(0), back_block(1)
    row = lax.broadcasted_iota(jnp.int32, (rows, 1), 0)
    step_keys = max(2, 128 // rows)

    def reach_of(b):
        if b < 0:
            return 0
        reach = min(n, (b + 1) * block * stride + 1)
        return min(n, -(-reach // step_keys) * step_keys)

    def at(c):
        return pl.ds(pl.multiple_of(c * rows, rows), rows)

    def settled_sum(a, c):
        return dka[at(c)] * scale if a == 0 else dva[at(c)]

    def hand_over(step, lo, hi):
        def act(i):
            for a in range(2):
                dkv[a, i, 1 - sub] = settled_sum(a, 2 * i + 1 - sub).astype(bf)

        each(lo // 2, hi // 2, act)
        span = pl.ds(lo // 2, (hi - lo) // 2)
        remote(dkv.at[:, span, 1 - sub], xkv.at[:, span], send_m.at[step], recv_m.at[step], mate).start()

    def send_home(step, lo, hi):
        came_in(recv_m.at[step], hi - lo)

        def act(i):
            for a, make in enumerate((back_k, back_v)):
                dkv[a, i, sub] = (settled_sum(a, 2 * i + sub) + xkv[a, i].astype(f32)).astype(bf)
                other, copy = make(i)
                pl.when(other != me)(copy.start)

        each(lo // 2, hi // 2, act)

    steps = list(reversed(range(heads // block)))
    but_own(came_in, recv_x.at[0], pairs)
    forward(0, kb).start()
    but_own(came_in, recv_x.at[2], heads)
    came_in(recv_f.at[0], pairs)
    for b in steps:
        lo, reach = b * block, reach_of(b)
        keys = reach * rows
        q = qb[pl.ds(lo, block)].reshape(block * rows, HD)
        k = kb[pl.ds(0, reach // 2)].reshape(keys, HD)
        qid = jnp.concatenate([numbers((lo + j) * stride + offset, row) for j in range(block)], axis=0)
        allowed = qid >= kid[:, :keys]
        score = lax.dot_general(q, k, over_last, preferred_element_type=f32) * scale
        score = jnp.where(allowed, score, -jnp.inf)
        top = jnp.max(score, axis=1, keepdims=True)
        e = jnp.exp(score - top)
        pa[b, :, pl.ds(0, keys)] = e * (1.0 / jnp.sum(e, axis=1, keepdims=True))
    but_own(came_in, recv_x.at[1], pairs)
    forward(1, vb).start()
    came_in(recv_f.at[1], pairs)
    for b in steps:
        lo, reach = b * block, reach_of(b)
        keys = reach * rows
        v = vb[pl.ds(0, reach // 2)].reshape(keys, HD)
        out = jnp.dot(pa[b, :, pl.ds(0, keys)].astype(bf), v, preferred_element_type=f32).astype(bf)
        ob[pl.ds(lo, block)] = out.reshape(block, rows, HD)
        start_each(lo, lo + block, back_o)
    but_own(came_in, recv_x.at[3], heads)
    late = None
    for b in steps:
        lo = b * block
        reach, settled = reach_of(b), reach_of(b - 1)
        keys = reach * rows
        q = qb[pl.ds(lo, block)].reshape(block * rows, HD)
        g = gb[pl.ds(lo, block)].reshape(block * rows, HD)
        k = kb[pl.ds(0, reach // 2)].reshape(keys, HD)
        v = vb[pl.ds(0, reach // 2)].reshape(keys, HD)
        out = ob[pl.ds(lo, block)].reshape(block * rows, HD)
        prob = pa[b, :, pl.ds(0, keys)]
        delta = jnp.sum(g.astype(f32) * out.astype(f32), axis=1, keepdims=True)
        dprob = lax.dot_general(g, v, over_last, preferred_element_type=f32)
        dscore = (prob * (dprob - delta)).astype(bf)
        dq = (jnp.dot(dscore, k, preferred_element_type=f32) * scale).astype(bf)
        dqb[pl.ds(lo, block)] = dq.reshape(block, rows, HD)
        dka[pl.ds(0, keys)] += lax.dot_general(dscore, q, over_first, preferred_element_type=f32)
        dva[pl.ds(0, keys)] += lax.dot_general(prob.astype(bf), g, over_first, preferred_element_type=f32)
        start_each(lo, lo + block, back_q)
        if reach > settled:
            hand_over(b, settled, reach)
        if late is not None:
            send_home(*late)
        late = (b, settled, reach) if reach > settled else None
    if late is not None:
        send_home(*late)

    @pl.when(parity == sub)
    def _():
        o_in[:, mine] = ob[slot]
        dq_in[:, mine] = dqb[slot]
        for a in range(2):
            dkv_in[a, my_group, :, mine] = dkv[a, place, parity]

    but_own(came_in, recv_o.at[0], heads)
    attn_ref[...] = o_in[...]
    partial = jnp.zeros((rows, pooled.shape[1]), f32)
    for s in reversed(range(chunks)):
        chunk = order(s)
        span = cols(chunk * per, per)
        blocks = per + 2 * per * groups
        own_chunk = at_home & (chunk == my_head // per)
        pl.when(own_chunk)(lambda: came_in(recv_b.at[chunk], blocks - 3))
        pl.when(jnp.logical_not(own_chunk))(lambda: came_in(recv_b.at[chunk], blocks))
        for j in range(3):
            if j == 0:
                summed = dq_in[:, span]
            elif groups == 1:
                summed = dkv_in[j - 1, 0, :, span]
            else:
                summed = dkv_in[j - 1, 0, :, span].astype(f32)
                for i in range(1, groups):
                    summed = summed + dkv_in[j - 1, i, :, span].astype(f32)
                summed = summed.astype(bf)
            partial += lax.dot_general(summed, wbuf[j, :, span], over_last, preferred_element_type=f32)
    for t in range(tp):
        part[t] = partial[:, t * width : (t + 1) * width].astype(bf)
    edge_lo, edge_hi = pl.ds(0, half), pl.ds(rows - half, half)
    def give_back(a, piece, into, peer):
        return [
            remote(piece(t), into.at[mt], send_r.at[a], recv_r.at[a], (peer, t))
            for t in (lax.rem(mt + i, tp) for i in range(1 if a == 2 else 0, tp))
        ]

    @pl.when(has_left)
    def _():
        for copy in give_back(0, lambda t: part.at[t, edge_lo], hi_part, left):
            copy.start()

    @pl.when(has_right)
    def _():
        for copy in give_back(1, lambda t: part.at[t, edge_hi], lo_part, right):
            copy.start()

    for copy in give_back(2, lambda t: part.at[t], own_part, me):
        copy.start()
    own_part[mt] = part[mt]
    target = jnp.where(
        pob < low,
        half - low + pob,
        jnp.where(pob >= count - high, half + rows + pob - (count - high), half + below + pob - low),
    )
    chooser = (target == lax.broadcasted_iota(jnp.int32, (2 * rows, 1), 0)).astype(f32)
    sizes = jnp.maximum(jnp.sum(chooser, axis=1, keepdims=True), 1.0)
    pl.when(has_left)(to_left.wait_send)
    pl.when(has_right)(to_right.wait_send)
    for a in range(2):
        but_own(went_out, send_x.at[a], pairs)
        but_own(went_out, send_x.at[2 + a], heads)
        but_own(went_out, send_h.at[a], heads)
        but_own(went_out, send_h.at[2 + a], pairs)
        went_out(send_f.at[a], pairs)
    for b in steps:
        if reach_of(b) > reach_of(b - 1):
            went_out(send_m.at[b], reach_of(b) - reach_of(b - 1))
    others = own_part.at[pl.ds(0, tp - 1)]
    for here, a, ref in ((has_right, 0, hi_part), (has_left, 1, lo_part)):
        pl.when(here)(lambda: remote(ref, ref, send_r.at[a], recv_r.at[a], mate).wait_recv())
    remote(others, others, send_r.at[2], recv_r.at[2], mate).wait_recv()
    for here, a, ref in ((has_left, 0, hi_part), (has_right, 1, lo_part)):
        pl.when(here)(lambda: remote(ref, ref, send_r.at[a], recv_r.at[a], mate).wait_send())
    remote(others, others, send_r.at[2], recv_r.at[2], mate).wait_send()

    def over_tp(ref):
        value = ref[0].astype(f32)
        for i in range(1, tp):
            value = value + ref[i].astype(f32)
        return value

    returned = jnp.concatenate([over_tp(lo_part), over_tp(own_part), over_tp(hi_part)], axis=0)
    shares = (returned.astype(bf).astype(f32) / sizes).astype(bf)
    grad_ref[...] = lax.dot_general(
        chooser.astype(bf), shares, over_first, preferred_element_type=f32
    ).astype(bf)


def emit_kernel(a_ref, g_ref, a_out, g_out, sem):
    copies = [
        pltpu.make_async_copy(src, dst, sem.at[i]) for i, (src, dst) in enumerate(((a_ref, a_out), (g_ref, g_out)))
    ]
    for copy in copies:
        copy.start()
    for copy in copies:
        copy.wait()


def shards(byte_states, patch_of_byte, patch_first, moved, w_qkv, d_attn):
    n, tp = lax.axis_size("ctx"), lax.axis_size("tp")
    rows, feats = d_attn.shape
    size, model = byte_states.shape
    heads = feats // HD
    pairs = n // 2
    groups = pairs // heads
    total = n * rows
    half = rows // 2
    width = model // tp
    block = per = 2 if heads % 2 == 0 else 1
    steps = heads // block
    assert tp % 2 == 0 and n % 2 == 0 and pairs % heads == 0
    bf, f32, i32 = jnp.bfloat16, jnp.float32, jnp.int32
    dma = pltpu.SemaphoreType.DMA
    results = pl.pallas_call(
        functools.partial(whole_kernel, n, tp, heads, rows, block, per),
        out_shape=[pltpu.VMEM((rows, feats), bf), pltpu.VMEM((size, width), bf)],
        in_specs=[ANY] * 6,
        out_specs=[VM] * 2,
        scratch_shapes=[
            pltpu.VMEM((size, model), bf), pltpu.VMEM((1, size), i32),
            pltpu.SMEM((n,), i32), pltpu.SMEM((2, n), i32),
            pltpu.VMEM(w_qkv.shape, bf), pltpu.VMEM((rows, feats), bf),
            pltpu.VMEM((2, half, model), bf), pltpu.VMEM((2, half, model), bf),
            pltpu.VMEM((rows, model), bf), pltpu.VMEM((3, rows, feats), bf),
            pltpu.VMEM((heads, rows, HD), bf), pltpu.VMEM((heads, rows, HD), bf),
            pltpu.VMEM((pairs, 2, rows, HD), bf), pltpu.VMEM((pairs, 2, rows, HD), bf),
            pltpu.VMEM((steps, block * rows, total), f32),
            pltpu.VMEM((heads, rows, HD), bf), pltpu.VMEM((heads, rows, HD), bf),
            pltpu.VMEM((2, pairs, 2, rows, HD), bf), pltpu.VMEM((2, pairs, rows, HD), bf),
            pltpu.VMEM((total, HD), f32), pltpu.VMEM((total, HD), f32),
            pltpu.VMEM((rows, feats), bf), pltpu.VMEM((rows, feats), bf),
            pltpu.VMEM((2, groups, rows, feats), bf),
            pltpu.VMEM((tp, rows, width), bf), pltpu.VMEM((tp, rows, width), bf),
            pltpu.VMEM((tp, half, width), bf), pltpu.VMEM((tp, half, width), bf),
            pltpu.VMEM((max(n, per + 2 * per * groups), rows, HD), bf),
            dma((5,)), dma((3,)), dma((2,)), dma((2,)), dma((4,)), dma((4,)), dma((2,)), dma((2,)),
            dma((steps,)), dma((steps,)), dma((4,)), dma((1,)), dma((heads // per,)), dma((3,)), dma((3,)),
        ],
        compiler_params=pltpu.CompilerParams(
            collective_id=0, has_side_effects=True, vmem_limit_bytes=60 << 20
        ),
        name="whole",
    )(byte_states, patch_of_byte.reshape(1, size), patch_first, moved, w_qkv, d_attn)
    results = [pltpu.with_memory_space_constraint(x, pltpu.VMEM) for x in results]
    return tuple(pl.pallas_call(
        emit_kernel,
        out_shape=[jax.ShapeDtypeStruct((rows, feats), bf), jax.ShapeDtypeStruct((size, width), bf)],
        in_specs=[VM, VM],
        out_specs=[ANY] * 2,
        scratch_shapes=[dma((2,))],
        name="emit",
    )(*results))


def solution(mesh):
    placed = (P("ctx", None), P("ctx"), P(), P(), P(None, None, "tp"), P("ctx", "tp"))
    return jax.shard_map(
        shards,
        mesh=mesh,
        in_specs=placed,
        out_specs=(P("ctx", "tp"), P("ctx", "tp")),
        check_vma=False,
    )
```

```python
import functools

import jax
import jax.numpy as jnp
from jax import lax
from jax.experimental import pallas as pl
from jax.experimental.pallas import tpu as pltpu
from jax.sharding import PartitionSpec as P

HD = 128
MESH = pl.DeviceIdType.MESH
VM = pl.BlockSpec(memory_space=pltpu.VMEM)
ANY = pl.BlockSpec(memory_space=pl.ANY)


def remote(src, dst, send, recv, device):
    return pltpu.make_async_remote_copy(
        src_ref=src, dst_ref=dst, send_sem=send, recv_sem=recv, device_id=device, device_id_type=MESH
    )


def each(lo, hi, act):
    def body(i, carry):
        act(i)
        return carry

    lax.fori_loop(lo, hi, body, 0)


def whole_kernel(
    n, tp, heads, rows, block, per,
    bytes_hbm, pob_hbm, first_hbm, moved_hbm, w_hbm, d_hbm,
    attn_ref, grad_ref,
    bytes_ref, pob_ref, first_ref, moved_ref, wbuf, d_ref,
    blk, came, pooled, own3, qb, gb, kb, vb, pa, ob, dqb, dkv, xkv, dka, dva,
    o_in, dq_in, dkv_in, part, own_part, lo_part, hi_part, tally,
    in_sem, w_sem, send_nb, recv_nb, send_x, recv_x, send_f, recv_f, send_m, recv_m,
    send_h, recv_o, recv_b, send_r, recv_r,
):
    pairs = n // 2
    groups = pairs // heads
    stride = 2 * groups
    total = n * rows
    half = rows // 2
    scale = HD ** (-0.5)
    bf, f32 = jnp.bfloat16, jnp.float32
    me, mt = lax.axis_index("ctx"), lax.axis_index("tp")
    sub = lax.rem(mt, 2)
    base = mt - sub
    mate = (me, base + 1 - sub)
    parity, place = lax.rem(me, 2), me // 2
    source_tp = base + parity
    at_home = parity == sub
    my_head, my_group = place // groups, lax.rem(place, groups)
    offset = 2 * my_group + sub
    slot = me // stride
    left, right = lax.rem(me + n - 1, n), lax.rem(me + 1, n)
    has_left, has_right = me > 0, me < n - 1
    width = part.shape[2]

    def cols(head, count=1):
        return pl.ds(pl.multiple_of(head * HD, HD), count * HD)

    chunks = heads // per

    def order(s):
        if chunks % 2:
            return lax.rem(my_head // per + (chunks + 1) // 2 + s, chunks)
        here, mid = my_head // per, chunks // 2
        upper = here // mid
        if s < mid:
            return (1 - upper) * (chunks - 1 - s) + upper * s
        back = chunks - 1 - s
        return upper * mid + lax.rem(here + back, mid)

    barrier = pltpu.get_barrier_semaphore()

    def greet(i):
        peer = lax.rem(me + i, n)
        for core in range(2):
            pl.semaphore_signal(barrier, inc=1, device_id=(peer, base + core), device_id_type=MESH)

    pl.semaphore_signal(barrier, inc=1, device_id=mate, device_id_type=MESH)
    each(1, n, greet)
    for c in (me, left, right):
        for i in range(2, tp):
            pl.semaphore_signal(
                barrier, inc=1, device_id=(c, lax.rem(base + i, tp)), device_id_type=MESH
            )
    inputs = [
        pltpu.make_async_copy(src, dst, in_sem.at[i])
        for i, (src, dst) in enumerate((
            (pob_hbm, pob_ref), (first_hbm, first_ref), (moved_hbm, moved_ref), (bytes_hbm, bytes_ref),
            (d_hbm, d_ref),
        ))
    ]
    for copy in inputs:
        copy.start()
    loads = [pltpu.make_async_copy(w_hbm.at[j], wbuf.at[j], w_sem.at[j]) for j in range(3)]
    for copy in inputs[:3]:
        copy.wait()

    def plan(c):
        below = moved_ref[1, lax.rem(c + n - 1, n)]
        above = moved_ref[0, lax.rem(c + 1, n)]
        start = first_ref[c]
        end = jnp.where(c == n - 1, total, first_ref[lax.rem(c + 1, n)])
        return start, end, below, above, moved_ref[0, c], moved_ref[1, c]

    def numbers(c, rank):
        start, end, below, above, low, high = plan(c)
        return jnp.where(
            rank < below,
            start - below + rank,
            jnp.where(rank >= rows - above, end + rank - (rows - above), start + low + rank - below),
        )

    start, end, below, above, low, high = plan(me)
    count = end - start
    rank = lax.broadcasted_iota(jnp.int32, (2 * rows, 1), 0)
    own_rank = rank - 2 * half
    own_local = jnp.where((own_rank >= below) & (own_rank < rows - above), low + own_rank - below, -1)
    up = jnp.where(rank - half < high, count - high + rank - half, -1)
    wanted = jnp.where(rank < half, rank - half + low, jnp.where(rank < 2 * half, up, own_local))
    pob = pob_ref[...]
    member = (pob == wanted).astype(f32)
    lengths = jnp.maximum(jnp.sum(member, axis=1, keepdims=True), 1.0)
    inputs[3].wait()
    for j in (1, 2, 0):
        loads[j].start()
    means = (
        jnp.dot(member.astype(bf), bytes_ref[...], preferred_element_type=f32) / lengths
    ).astype(bf)
    blk[0] = means[:half]
    blk[1] = means[half : 2 * half]

    @pl.when(me == 0)
    def _():
        came[1] = jnp.zeros_like(came[1])
        lo_part[...] = jnp.zeros_like(lo_part)

    @pl.when(me == n - 1)
    def _():
        came[0] = jnp.zeros_like(came[0])
        hi_part[...] = jnp.zeros_like(hi_part)

    pl.semaphore_wait(barrier, 2 * n - 1 + 3 * (tp - 2))
    to_left = remote(blk.at[0], came.at[0], send_nb.at[0], recv_nb.at[0], (left, mt))
    to_right = remote(blk.at[1], came.at[1], send_nb.at[1], recv_nb.at[1], (right, mt))
    pl.when(has_left)(to_left.start)
    pl.when(has_right)(to_right.start)

    def amount(count):
        return tally.at[pl.ds(0, count)]

    def came_in(sem, count):
        remote(amount(count), amount(count), sem, sem, mate).wait_recv()

    def went_out(sem, count):
        remote(amount(count), amount(count), sem, sem, mate).wait_send()

    def but_own(wait, sem, count, own=1):
        pl.when(at_home)(lambda: wait(sem, count - own))
        pl.when(jnp.logical_not(at_home))(lambda: wait(sem, count))

    def start_each(lo, hi, make):
        def act(i):
            other, copy = make(i)
            pl.when(other != me)(copy.start)

        each(lo, hi, act)

    def send_block(a, ref, out):
        def make(i):
            chip = 2 * i + sub
            return chip, remote(
                ref.at[:, cols(i // groups)], out.at[place, parity], send_x.at[a], recv_x.at[a],
                (chip, base + parity),
            )

        return make

    def send_query(a, ref, out):
        def make(h):
            chip = 2 * (h * groups + my_group) + sub
            return chip, remote(
                ref.at[:, cols(h)], out.at[slot], send_x.at[a], recv_x.at[a], (chip, base + parity)
            )

        return make

    def forward(a, ref):
        return remote(ref.at[:, sub], ref.at[:, sub], send_f.at[a], recv_f.at[a], mate)

    def back_query(a, ref, out):
        def make(j):
            c = j * stride + offset
            return c, remote(
                ref.at[j], out.at[:, cols(my_head)], send_h.at[a], recv_o.at[a], (c, source_tp)
            )

        return make

    def back_block(a):
        def make(i):
            c = 2 * i + sub
            return c, remote(
                dkv.at[a, i, sub], dkv_in.at[a, my_group, :, cols(my_head)], send_h.at[2 + a],
                recv_b.at[my_head // per], (c, source_tp),
            )

        return make

    send_g, send_q = send_query(3, d_ref, gb), send_query(2, own3.at[0], qb)
    send_k, send_v = send_block(0, own3.at[1], kb), send_block(1, own3.at[2], vb)
    inputs[4].wait()
    early = chunks // 2
    for s in range(early):
        start_each(order(s) * per, order(s) * per + per, send_g)
    lane = lax.broadcasted_iota(jnp.int32, (1, total), 1)

    def number_keys(c, ids):
        return jnp.where((lane >= c * rows) & (lane < (c + 1) * rows), numbers(c, lane - c * rows), ids)

    kid = lax.fori_loop(0, n, number_keys, jnp.zeros((1, total), jnp.int32))
    dka[...] = jnp.zeros_like(dka)
    dva[...] = jnp.zeros_like(dva)
    pl.when(has_left)(to_right.wait_recv)
    pl.when(has_right)(to_left.wait_recv)
    pooled[pl.ds(0, half)] = means[2 * half : 3 * half] + came[1]
    pooled[pl.ds(half, half)] = means[3 * half :] + came[0]
    mine = cols(my_head)
    for j, make in ((1, send_k), (2, send_v), (0, send_q)):
        loads[j].wait()
        for s in range(chunks):
            chunk = order(s)
            span = cols(chunk * per, per)
            own3[j, :, span] = jnp.dot(
                pooled[...], wbuf[j, :, span], preferred_element_type=f32
            ).astype(bf)
            each_head = per if j == 0 else per * groups
            start_each(chunk * each_head, (chunk + 1) * each_head, make)
    for s in range(early, chunks):
        start_each(order(s) * per, order(s) * per + per, send_g)

    @pl.when(parity == sub)
    def _():
        qb[slot] = own3[0, :, mine]
        kb[place, parity] = own3[1, :, mine]
        vb[place, parity] = own3[2, :, mine]
        gb[slot] = d_ref[:, mine]

    over_last = (((1,), (1,)), ((), ()))
    over_first = (((0,), (0,)), ((), ()))
    back_o, back_q = back_query(0, ob, o_in), back_query(1, dqb, dq_in)
    back_k, back_v = back_block(0), back_block(1)
    row = lax.broadcasted_iota(jnp.int32, (rows, 1), 0)
    step_keys = max(2, 128 // rows)

    def reach_of(b):
        if b < 0:
            return 0
        reach = min(n, (b + 1) * block * stride + 1)
        return min(n, -(-reach // step_keys) * step_keys)

    def at(c):
        return pl.ds(pl.multiple_of(c * rows, rows), rows)

    def settled_sum(a, c):
        return dka[at(c)] * scale if a == 0 else dva[at(c)]

    def hand_over(step, lo, hi):
        def act(i):
            for a in range(2):
                dkv[a, i, 1 - sub] = settled_sum(a, 2 * i + 1 - sub).astype(bf)

        each(lo // 2, hi // 2, act)
        span = pl.ds(lo // 2, (hi - lo) // 2)
        remote(dkv.at[:, span, 1 - sub], xkv.at[:, span], send_m.at[step], recv_m.at[step], mate).start()

    def send_home(step, lo, hi):
        came_in(recv_m.at[step], hi - lo)

        def act(i):
            for a, make in enumerate((back_k, back_v)):
                dkv[a, i, sub] = (settled_sum(a, 2 * i + sub) + xkv[a, i].astype(f32)).astype(bf)
                other, copy = make(i)
                pl.when(other != me)(copy.start)

        each(lo // 2, hi // 2, act)

    steps = list(reversed(range(heads // block)))
    but_own(came_in, recv_x.at[0], pairs)
    forward(0, kb).start()
    but_own(came_in, recv_x.at[1], pairs)
    forward(1, vb).start()
    but_own(came_in, recv_x.at[2], heads)
    came_in(recv_f.at[0], pairs)
    came_in(recv_f.at[1], pairs)

    def attend(b):
        lo, reach = b * block, reach_of(b)
        keys = reach * rows
        q = qb[pl.ds(lo, block)].reshape(block * rows, HD)
        k = kb[pl.ds(0, reach // 2)].reshape(keys, HD)
        v = vb[pl.ds(0, reach // 2)].reshape(keys, HD)
        qid = jnp.concatenate([numbers((lo + j) * stride + offset, row) for j in range(block)], axis=0)
        allowed = qid >= kid[:, :keys]
        score = lax.dot_general(q, k, over_last, preferred_element_type=f32) * scale
        score = jnp.where(allowed, score, -jnp.inf)
        top = jnp.max(score, axis=1, keepdims=True)
        e = jnp.exp(score - top)
        prob = e * (1.0 / jnp.sum(e, axis=1, keepdims=True))
        pa[b, :, pl.ds(0, keys)] = prob
        out = jnp.dot(prob.astype(bf), v, preferred_element_type=f32).astype(bf)
        ob[pl.ds(lo, block)] = out.reshape(block, rows, HD)
        start_each(lo, lo + block, back_o)

    def differentiate(b):
        lo = b * block
        keys = reach_of(b) * rows
        q = qb[pl.ds(lo, block)].reshape(block * rows, HD)
        g = gb[pl.ds(lo, block)].reshape(block * rows, HD)
        k = kb[pl.ds(0, reach_of(b) // 2)].reshape(keys, HD)
        v = vb[pl.ds(0, reach_of(b) // 2)].reshape(keys, HD)
        out = ob[pl.ds(lo, block)].reshape(block * rows, HD)
        prob = pa[b, :, pl.ds(0, keys)]
        delta = jnp.sum(g.astype(f32) * out.astype(f32), axis=1, keepdims=True)
        dprob = lax.dot_general(g, v, over_last, preferred_element_type=f32)
        dscore = (prob * (dprob - delta)).astype(bf)
        dq = (jnp.dot(dscore, k, preferred_element_type=f32) * scale).astype(bf)
        dqb[pl.ds(lo, block)] = dq.reshape(block, rows, HD)
        start_each(lo, lo + block, back_q)
        dka[pl.ds(0, keys)] += lax.dot_general(dscore, q, over_first, preferred_element_type=f32)
        dva[pl.ds(0, keys)] += lax.dot_general(prob.astype(bf), g, over_first, preferred_element_type=f32)

    middle = n // 2 // step_keys * step_keys
    whole = [(i, lo, hi) for i, (lo, hi) in enumerate(((0, middle), (middle, n))) if hi > lo]
    falling = (steps, {b: [(b, reach_of(b - 1), reach_of(b))] for b in steps if reach_of(b) > reach_of(b - 1)})
    rising = (steps[::-1], {steps[0]: whole})
    upper = me >= n // 2
    halves = [(upper, rising), (jnp.logical_not(upper), falling)] if len(steps) > 1 else [(me >= 0, falling)]

    def work(blocks, spans):
        for b in blocks:
            attend(b)
        but_own(came_in, recv_x.at[3], heads)
        late = []
        for b in blocks:
            differentiate(b)
            for span in spans.get(b, ()):
                hand_over(*span)
            for span in late:
                send_home(*span)
            late = spans.get(b, [])
        for span in late:
            send_home(*span)

    for here, plan_of in halves:
        pl.when(here)(functools.partial(work, *plan_of))

    @pl.when(parity == sub)
    def _():
        o_in[:, mine] = ob[slot]
        dq_in[:, mine] = dqb[slot]
        for a in range(2):
            dkv_in[a, my_group, :, mine] = dkv[a, place, parity]

    but_own(came_in, recv_o.at[0], heads)
    attn_ref[...] = o_in[...]
    but_own(came_in, recv_o.at[1], heads)
    partial = lax.dot_general(dq_in[...], wbuf[0], over_last, preferred_element_type=f32)
    for s in reversed(range(chunks)):
        chunk = order(s)
        span = cols(chunk * per, per)
        blocks = 2 * per * groups
        own_chunk = at_home & (chunk == my_head // per)
        pl.when(own_chunk)(lambda: came_in(recv_b.at[chunk], blocks - 2))
        pl.when(jnp.logical_not(own_chunk))(lambda: came_in(recv_b.at[chunk], blocks))
        for j in (1, 2):
            if groups == 1:
                summed = dkv_in[j - 1, 0, :, span]
            else:
                summed = dkv_in[j - 1, 0, :, span].astype(f32)
                for i in range(1, groups):
                    summed = summed + dkv_in[j - 1, i, :, span].astype(f32)
                summed = summed.astype(bf)
            partial += lax.dot_general(summed, wbuf[j, :, span], over_last, preferred_element_type=f32)
    for t in range(tp):
        part[t] = partial[:, t * width : (t + 1) * width].astype(bf)
    edge_lo, edge_hi = pl.ds(0, half), pl.ds(rows - half, half)
    def give_back(a, piece, into, peer):
        return [
            remote(piece(t), into.at[mt], send_r.at[a], recv_r.at[a], (peer, t))
            for t in (lax.rem(mt + i, tp) for i in range(1 if a == 2 else 0, tp))
        ]

    @pl.when(has_left)
    def _():
        for copy in give_back(0, lambda t: part.at[t, edge_lo], hi_part, left):
            copy.start()

    @pl.when(has_right)
    def _():
        for copy in give_back(1, lambda t: part.at[t, edge_hi], lo_part, right):
            copy.start()

    for copy in give_back(2, lambda t: part.at[t], own_part, me):
        copy.start()
    own_part[mt] = part[mt]
    target = jnp.where(
        pob < low,
        half - low + pob,
        jnp.where(pob >= count - high, half + rows + pob - (count - high), half + below + pob - low),
    )
    chooser = (target == lax.broadcasted_iota(jnp.int32, (2 * rows, 1), 0)).astype(f32)
    sizes = jnp.maximum(jnp.sum(chooser, axis=1, keepdims=True), 1.0)
    pl.when(has_left)(to_left.wait_send)
    pl.when(has_right)(to_right.wait_send)
    for a in range(2):
        but_own(went_out, send_x.at[a], pairs)
        but_own(went_out, send_x.at[2 + a], heads)
        but_own(went_out, send_h.at[a], heads)
        but_own(went_out, send_h.at[2 + a], pairs)
        went_out(send_f.at[a], pairs)

    def handed_over(blocks, spans):
        for b in blocks:
            for i, lo, hi in spans.get(b, ()):
                went_out(send_m.at[i], hi - lo)

    for here, plan_of in halves:
        pl.when(here)(functools.partial(handed_over, *plan_of))
    others = own_part.at[pl.ds(0, tp - 1)]
    for here, a, ref in ((has_right, 0, hi_part), (has_left, 1, lo_part)):
        pl.when(here)(lambda: remote(ref, ref, send_r.at[a], recv_r.at[a], mate).wait_recv())
    remote(others, others, send_r.at[2], recv_r.at[2], mate).wait_recv()
    for here, a, ref in ((has_left, 0, hi_part), (has_right, 1, lo_part)):
        pl.when(here)(lambda: remote(ref, ref, send_r.at[a], recv_r.at[a], mate).wait_send())
    remote(others, others, send_r.at[2], recv_r.at[2], mate).wait_send()

    def over_tp(ref):
        value = ref[0].astype(f32)
        for i in range(1, tp):
            value = value + ref[i].astype(f32)
        return value

    returned = jnp.concatenate([over_tp(lo_part), over_tp(own_part), over_tp(hi_part)], axis=0)
    shares = (returned.astype(bf).astype(f32) / sizes).astype(bf)
    grad_ref[...] = lax.dot_general(
        chooser.astype(bf), shares, over_first, preferred_element_type=f32
    ).astype(bf)


def emit_kernel(a_ref, g_ref, a_out, g_out, sem):
    copies = [
        pltpu.make_async_copy(src, dst, sem.at[i]) for i, (src, dst) in enumerate(((a_ref, a_out), (g_ref, g_out)))
    ]
    for copy in copies:
        copy.start()
    for copy in copies:
        copy.wait()


def shards(byte_states, patch_of_byte, patch_first, moved, w_qkv, d_attn):
    n, tp = lax.axis_size("ctx"), lax.axis_size("tp")
    rows, feats = d_attn.shape
    size, model = byte_states.shape
    heads = feats // HD
    pairs = n // 2
    groups = pairs // heads
    total = n * rows
    half = rows // 2
    width = model // tp
    block = per = 2 if heads % 2 == 0 else 1
    steps = heads // block
    assert tp % 2 == 0 and n % 2 == 0 and pairs % heads == 0
    bf, f32, i32 = jnp.bfloat16, jnp.float32, jnp.int32
    dma = pltpu.SemaphoreType.DMA
    results = pl.pallas_call(
        functools.partial(whole_kernel, n, tp, heads, rows, block, per),
        out_shape=[pltpu.VMEM((rows, feats), bf), pltpu.VMEM((size, width), bf)],
        in_specs=[ANY] * 6,
        out_specs=[VM] * 2,
        scratch_shapes=[
            pltpu.VMEM((size, model), bf), pltpu.VMEM((1, size), i32),
            pltpu.SMEM((n,), i32), pltpu.SMEM((2, n), i32),
            pltpu.VMEM(w_qkv.shape, bf), pltpu.VMEM((rows, feats), bf),
            pltpu.VMEM((2, half, model), bf), pltpu.VMEM((2, half, model), bf),
            pltpu.VMEM((rows, model), bf), pltpu.VMEM((3, rows, feats), bf),
            pltpu.VMEM((heads, rows, HD), bf), pltpu.VMEM((heads, rows, HD), bf),
            pltpu.VMEM((pairs, 2, rows, HD), bf), pltpu.VMEM((pairs, 2, rows, HD), bf),
            pltpu.VMEM((steps, block * rows, total), f32),
            pltpu.VMEM((heads, rows, HD), bf), pltpu.VMEM((heads, rows, HD), bf),
            pltpu.VMEM((2, pairs, 2, rows, HD), bf), pltpu.VMEM((2, pairs, rows, HD), bf),
            pltpu.VMEM((total, HD), f32), pltpu.VMEM((total, HD), f32),
            pltpu.VMEM((rows, feats), bf), pltpu.VMEM((rows, feats), bf),
            pltpu.VMEM((2, groups, rows, feats), bf),
            pltpu.VMEM((tp, rows, width), bf), pltpu.VMEM((tp, rows, width), bf),
            pltpu.VMEM((tp, half, width), bf), pltpu.VMEM((tp, half, width), bf),
            pltpu.VMEM((max(n, per + 2 * per * groups), rows, HD), bf),
            dma((5,)), dma((3,)), dma((2,)), dma((2,)), dma((4,)), dma((4,)), dma((2,)), dma((2,)),
            dma((max(2, steps),)), dma((max(2, steps),)), dma((4,)), dma((2,)), dma((heads // per,)), dma((3,)), dma((3,)),
        ],
        compiler_params=pltpu.CompilerParams(
            collective_id=0, has_side_effects=True, vmem_limit_bytes=60 << 20
        ),
        name="whole",
    )(byte_states, patch_of_byte.reshape(1, size), patch_first, moved, w_qkv, d_attn)
    results = [pltpu.with_memory_space_constraint(x, pltpu.VMEM) for x in results]
    return tuple(pl.pallas_call(
        emit_kernel,
        out_shape=[jax.ShapeDtypeStruct((rows, feats), bf), jax.ShapeDtypeStruct((size, width), bf)],
        in_specs=[VM, VM],
        out_specs=[ANY] * 2,
        scratch_shapes=[dma((2,))],
        name="emit",
    )(*results))


def solution(mesh):
    placed = (P("ctx", None), P("ctx"), P(), P(), P(None, None, "tp"), P("ctx", "tp"))
    return jax.shard_map(
        shards,
        mesh=mesh,
        in_specs=placed,
        out_specs=(P("ctx", "tp"), P("ctx", "tp")),
        check_vma=False,
    )
```

```python
import functools

import jax
import jax.numpy as jnp
from jax import lax
from jax.experimental import pallas as pl
from jax.experimental.pallas import tpu as pltpu
from jax.sharding import PartitionSpec as P

HD = 128
MESH = pl.DeviceIdType.MESH
VM = pl.BlockSpec(memory_space=pltpu.VMEM)
ANY = pl.BlockSpec(memory_space=pl.ANY)


def remote(src, dst, send, recv, device):
    return pltpu.make_async_remote_copy(
        src_ref=src, dst_ref=dst, send_sem=send, recv_sem=recv, device_id=device, device_id_type=MESH
    )


def each(lo, hi, act):
    def body(i, carry):
        act(i)
        return carry

    lax.fori_loop(lo, hi, body, 0)


def whole_kernel(
    n, tp, heads, rows, block, per,
    bytes_hbm, pob_hbm, first_hbm, moved_hbm, w_hbm, d_hbm,
    attn_ref, grad_ref,
    bytes_ref, pob_ref, first_ref, moved_ref, wbuf, d_ref,
    blk, came, pooled, own3, qb, gb, kb, vb, pa, ob, dqb, dkv, xkv, dkva,
    o_in, dq_in, dkv_in, part, own_part, lo_part, hi_part, tally,
    in_sem, w_sem, send_nb, recv_nb, send_x, recv_x, recv_q, send_f, recv_f, send_m, recv_m,
    send_h, recv_o, recv_b, send_r, recv_r, word,
):
    pairs = n // 2
    groups = pairs // heads
    stride = 2 * groups
    total = n * rows
    half = rows // 2
    scale = HD ** (-0.5)
    bf, f32 = jnp.bfloat16, jnp.float32
    me, mt = lax.axis_index("ctx"), lax.axis_index("tp")
    sub = lax.rem(mt, 2)
    base = mt - sub
    mate = (me, base + 1 - sub)
    parity, place = lax.rem(me, 2), me // 2
    source_tp = base + parity
    at_home = parity == sub
    my_head, my_group = place // groups, lax.rem(place, groups)
    offset = 2 * my_group + sub
    slot = me // stride
    left, right = lax.rem(me + n - 1, n), lax.rem(me + 1, n)
    has_left, has_right = me > 0, me < n - 1
    width = part.shape[2]

    def cols(head, count=1):
        return pl.ds(pl.multiple_of(head * HD, HD), count * HD)

    chunks = heads // per

    def order(s):
        if chunks % 2:
            return lax.rem(my_head // per + (chunks + 1) // 2 + s, chunks)
        here, mid = my_head // per, chunks // 2
        upper = here // mid
        if s < mid:
            return (1 - upper) * (chunks - 1 - s) + upper * s
        back = chunks - 1 - s
        return upper * mid + lax.rem(here + back, mid)

    barrier = pltpu.get_barrier_semaphore()

    window = -(-n // 4)

    def greet(i):
        for there, peer in ((me >= i, me - i), (me + i < n, me + i)):
            @pl.when(there)
            def _():
                for core in range(2):
                    pl.semaphore_signal(barrier, inc=1, device_id=(peer, base + core), device_id_type=MESH)

    pl.semaphore_signal(barrier, inc=1, device_id=mate, device_id_type=MESH)
    each(1, window + 1, greet)
    for there, c in ((me >= 0, me), (has_left, me - 1), (has_right, me + 1)):
        for i in range(2, tp):
            pl.when(there)(functools.partial(
                pl.semaphore_signal, barrier, inc=1, device_id=(c, lax.rem(base + i, tp)), device_id_type=MESH
            ))
    beside = has_left.astype(jnp.int32) + has_right.astype(jnp.int32)
    expected = 1 + 2 * (jnp.minimum(me, window) + jnp.minimum(n - 1 - me, window)) + (tp - 2) * (1 + beside)

    def spread(round_):
        far = window << round_
        for there, peer in ((me >= far, me - far), (me + far < n, me + far)):
            pl.when(there)(functools.partial(
                pl.semaphore_signal, word.at[round_], inc=1, device_id=(peer, mt), device_id_type=MESH
            ))

    def heard(round_):
        far = window << round_
        pl.semaphore_wait(word.at[round_], (me >= far).astype(jnp.int32) + (me + far < n).astype(jnp.int32))

    inputs = [
        pltpu.make_async_copy(src, dst, in_sem.at[i])
        for i, (src, dst) in enumerate((
            (pob_hbm, pob_ref), (first_hbm, first_ref), (moved_hbm, moved_ref), (bytes_hbm, bytes_ref),
            (d_hbm, d_ref),
        ))
    ]
    for copy in inputs:
        copy.start()
    loads = [pltpu.make_async_copy(w_hbm.at[j], wbuf.at[j], w_sem.at[j]) for j in range(3)]
    for copy in inputs[:3]:
        copy.wait()

    def plan(c):
        below = moved_ref[1, lax.rem(c + n - 1, n)]
        above = moved_ref[0, lax.rem(c + 1, n)]
        start = first_ref[c]
        end = jnp.where(c == n - 1, total, first_ref[lax.rem(c + 1, n)])
        return start, end, below, above, moved_ref[0, c], moved_ref[1, c]

    def numbers(c, rank):
        start, end, below, above, low, high = plan(c)
        return jnp.where(
            rank < below,
            start - below + rank,
            jnp.where(rank >= rows - above, end + rank - (rows - above), start + low + rank - below),
        )

    start, end, below, above, low, high = plan(me)
    count = end - start
    rank = lax.broadcasted_iota(jnp.int32, (2 * rows, 1), 0)
    own_rank = rank - 2 * half
    own_local = jnp.where((own_rank >= below) & (own_rank < rows - above), low + own_rank - below, -1)
    up = jnp.where(rank - half < high, count - high + rank - half, -1)
    wanted = jnp.where(rank < half, rank - half + low, jnp.where(rank < 2 * half, up, own_local))
    pob = pob_ref[...]
    member = (pob == wanted).astype(f32)
    lengths = jnp.maximum(jnp.sum(member, axis=1, keepdims=True), 1.0)
    inputs[3].wait()
    for j in (1, 2, 0):
        loads[j].start()
    means = (
        jnp.dot(member.astype(bf), bytes_ref[...], preferred_element_type=f32) / lengths
    ).astype(bf)
    blk[0] = means[:half]
    blk[1] = means[half : 2 * half]

    @pl.when(me == 0)
    def _():
        came[1] = jnp.zeros_like(came[1])
        lo_part[...] = jnp.zeros_like(lo_part)

    @pl.when(me == n - 1)
    def _():
        came[0] = jnp.zeros_like(came[0])
        hi_part[...] = jnp.zeros_like(hi_part)

    pl.semaphore_wait(barrier, expected)
    to_left = remote(blk.at[0], came.at[0], send_nb.at[0], recv_nb.at[0], (left, mt))
    to_right = remote(blk.at[1], came.at[1], send_nb.at[1], recv_nb.at[1], (right, mt))
    pl.when(has_left)(to_left.start)
    pl.when(has_right)(to_right.start)
    spread(0)
    heard(0)
    spread(1)

    def amount(count):
        return tally.at[pl.ds(0, count)]

    def came_in(sem, count):
        remote(amount(count), amount(count), sem, sem, mate).wait_recv()

    def went_out(sem, count):
        remote(amount(count), amount(count), sem, sem, mate).wait_send()

    def but_own(wait, sem, count, own=1):
        pl.when(at_home)(lambda: wait(sem, count - own))
        pl.when(jnp.logical_not(at_home))(lambda: wait(sem, count))

    def start_each(lo, hi, make):
        def act(i):
            other, copy = make(i)
            pl.when(other != me)(copy.start)

        each(lo, hi, act)

    def send_block(a, ref, out):
        def make(i):
            chip = 2 * i + sub
            return chip, remote(
                ref.at[:, cols(i // groups)], out.at[place, parity], send_x.at[a], recv_x.at[a],
                (chip, base + parity),
            )

        return make

    def send_query(a, ref, out):
        def make(h):
            chip = 2 * (h * groups + my_group) + sub
            return chip, remote(
                ref.at[:, cols(h)], out.at[slot], send_x.at[a],
                recv_q.at[slot // block] if a == 2 else recv_x.at[a], (chip, base + parity),
            )

        return make

    def forward(a, ref):
        return remote(ref.at[:, sub], ref.at[:, sub], send_f.at[a], recv_f.at[a], mate)

    def back_query(a, ref, out):
        def make(j):
            c = j * stride + offset
            return c, remote(
                ref.at[j], out.at[:, cols(my_head)], send_h.at[a], recv_o.at[a], (c, source_tp)
            )

        return make

    def back_block(i):
        c = 2 * i + sub
        return c, remote(
            dkv.at[:, i, sub], dkv_in.at[:, my_group, :, cols(my_head)], send_h.at[2],
            recv_b.at[my_head // per], (c, source_tp),
        )

    send_g, send_q = send_query(3, d_ref, gb), send_query(2, own3.at[0], qb)
    send_k, send_v = send_block(0, own3.at[1], kb), send_block(1, own3.at[2], vb)
    heard(1)
    inputs[4].wait()
    early = chunks // 2
    for s in range(early):
        start_each(order(s) * per, order(s) * per + per, send_g)
    lane = lax.broadcasted_iota(jnp.int32, (1, total), 1)

    def number_keys(c, ids):
        return jnp.where((lane >= c * rows) & (lane < (c + 1) * rows), numbers(c, lane - c * rows), ids)

    kid = lax.fori_loop(0, n, number_keys, jnp.zeros((1, total), jnp.int32))
    pl.when(has_left)(to_right.wait_recv)
    pl.when(has_right)(to_left.wait_recv)
    pooled[pl.ds(0, half)] = means[2 * half : 3 * half] + came[1]
    pooled[pl.ds(half, half)] = means[3 * half :] + came[0]
    mine = cols(my_head)
    makers = (send_q, send_k, send_v)

    def project(kinds):
        for j, places in kinds:
            loads[j].wait()
            for s in places:
                span = cols(order(s) * per, per)
                own3[j, :, span] = jnp.dot(
                    pooled[...], wbuf[j, :, span], preferred_element_type=f32
                ).astype(bf)
                each_head = per if j == 0 else per * groups
                start_each(order(s) * each_head, (order(s) + 1) * each_head, makers[j])

    outer = (me < n // 4) | (me >= n - n // 4)
    far_first = list(range(chunks))
    project(((1, far_first), (2, far_first)))
    pl.when(outer)(lambda: project(((0, far_first),)))
    pl.when(jnp.logical_not(outer))(lambda: project(((0, far_first[::-1]),)))
    for s in range(early, chunks):
        start_each(order(s) * per, order(s) * per + per, send_g)

    @pl.when(parity == sub)
    def _():
        qb[slot] = own3[0, :, mine]
        kb[place, parity] = own3[1, :, mine]
        vb[place, parity] = own3[2, :, mine]
        gb[slot] = d_ref[:, mine]

    over_last = (((1,), (1,)), ((), ()))
    over_first = (((0,), (0,)), ((), ()))
    back_o, back_q = back_query(0, ob, o_in), back_query(1, dqb, dq_in)
    row = lax.broadcasted_iota(jnp.int32, (rows, 1), 0)
    step_keys = max(2, 128 // rows)

    def reach_of(b):
        if b < 0:
            return 0
        reach = min(n, (b + 1) * block * stride + 1)
        return min(n, -(-reach // step_keys) * step_keys)

    def at(c):
        return pl.ds(pl.multiple_of(c * rows, rows), rows)

    def settled_sum(a, c):
        value = dkva[at(c), a * HD : (a + 1) * HD]
        return value * scale if a == 0 else value

    def hand_over(step, lo, hi):
        def act(i):
            for a in range(2):
                dkv[a, i, 1 - sub] = settled_sum(a, 2 * i + 1 - sub).astype(bf)

        each(lo // 2, hi // 2, act)
        span = pl.ds(lo // 2, (hi - lo) // 2)
        remote(dkv.at[:, span, 1 - sub], xkv.at[:, span], send_m.at[step], recv_m.at[step], mate).start()

    def send_home(step, lo, hi):
        came_in(recv_m.at[step], hi - lo)

        def act(i):
            for a in range(2):
                dkv[a, i, sub] = (settled_sum(a, 2 * i + sub) + xkv[a, i].astype(f32)).astype(bf)
            other, copy = back_block(i)
            pl.when(other != me)(copy.start)

        each(lo // 2, hi // 2, act)

    steps = list(reversed(range(heads // block)))
    but_own(came_in, recv_x.at[0], pairs)
    forward(0, kb).start()
    but_own(came_in, recv_x.at[1], pairs)
    forward(1, vb).start()
    came_in(recv_f.at[0], pairs)
    came_in(recv_f.at[1], pairs)

    def attend(b):
        lo, reach = b * block, reach_of(b)
        keys = reach * rows
        q = qb[pl.ds(lo, block)].reshape(block * rows, HD)
        k = kb[pl.ds(0, reach // 2)].reshape(keys, HD)
        v = vb[pl.ds(0, reach // 2)].reshape(keys, HD)
        qid = jnp.concatenate([numbers((lo + j) * stride + offset, row) for j in range(block)], axis=0)
        allowed = qid >= kid[:, :keys]
        score = lax.dot_general(q, k, over_last, preferred_element_type=f32) * scale
        score = jnp.where(allowed, score, -jnp.inf)
        top = jnp.max(score, axis=1, keepdims=True)
        e = jnp.exp(score - top)
        prob = e * (1.0 / jnp.sum(e, axis=1, keepdims=True))
        pa[b, :, pl.ds(0, keys)] = prob
        out = jnp.dot(prob.astype(bf), v, preferred_element_type=f32).astype(bf)
        ob[pl.ds(lo, block)] = out.reshape(block, rows, HD)

    def differentiate(b, filled):
        lo = b * block
        keys = reach_of(b) * rows
        q = qb[pl.ds(lo, block)].reshape(block * rows, HD)
        g = gb[pl.ds(lo, block)].reshape(block * rows, HD)
        k = kb[pl.ds(0, reach_of(b) // 2)].reshape(keys, HD)
        v = vb[pl.ds(0, reach_of(b) // 2)].reshape(keys, HD)
        out = ob[pl.ds(lo, block)].reshape(block * rows, HD)
        prob = pa[b, :, pl.ds(0, keys)]
        delta = jnp.sum(g.astype(f32) * out.astype(f32), axis=1, keepdims=True)
        dprob = lax.dot_general(g, v, over_last, preferred_element_type=f32)
        dscore = (prob * (dprob - delta)).astype(bf)
        dq = (jnp.dot(dscore, k, preferred_element_type=f32) * scale).astype(bf)
        dqb[pl.ds(lo, block)] = dq.reshape(block, rows, HD)
        blank = jnp.zeros_like(q)
        both = lax.dot_general(
            jnp.concatenate([dscore, prob.astype(bf)], axis=0),
            jnp.concatenate(
                [jnp.concatenate([q, blank], axis=1), jnp.concatenate([blank, g], axis=1)], axis=0
            ),
            over_first, preferred_element_type=f32,
        )
        old = min(keys, filled)
        if old:
            dkva[pl.ds(0, old)] += both[:old]
        if keys > old:
            dkva[pl.ds(old, keys - old)] = both[old:]
        return max(keys, filled)

    middle = n // 2 // step_keys * step_keys
    whole = [(i, lo, hi) for i, (lo, hi) in enumerate(((0, middle), (middle, n))) if hi > lo]
    falling = (steps, {b: [(b, reach_of(b - 1), reach_of(b))] for b in steps if reach_of(b) > reach_of(b - 1)})
    rising = (steps[::-1], {steps[0]: whole})
    upper = me >= n // 2
    halves = [(upper, rising), (jnp.logical_not(upper), falling)] if len(steps) > 1 else [(me >= 0, falling)]

    def work(blocks, spans):
        lead, first = max(1, len(blocks) // 2), blocks[:1]
        for part_of in (first, blocks[1:]):
            for b in part_of:
                mine_too = at_home & (slot // block == b)
                pl.when(mine_too)(lambda: came_in(recv_q.at[b], block - 1))
                pl.when(jnp.logical_not(mine_too))(lambda: came_in(recv_q.at[b], block))
            for b in part_of:
                attend(b)
            for b in part_of:
                start_each(b * block, (b + 1) * block, back_o)
        but_own(came_in, recv_x.at[3], heads)
        late, filled = [], 0
        for part_of in (blocks[:lead], blocks[lead:]):
            for b in part_of:
                filled = differentiate(b, filled)
            for b in part_of:
                start_each(b * block, (b + 1) * block, back_q)
            ready = [span for b in part_of for span in spans.get(b, ())]
            for span in ready:
                hand_over(*span)
            for span in late:
                send_home(*span)
            late = ready
        for span in late:
            send_home(*span)

    for here, plan_of in halves:
        pl.when(here)(functools.partial(work, *plan_of))

    @pl.when(parity == sub)
    def _():
        o_in[:, mine] = ob[slot]
        dq_in[:, mine] = dqb[slot]
        for a in range(2):
            dkv_in[a, my_group, :, mine] = dkv[a, place, parity]

    but_own(came_in, recv_o.at[0], heads)
    attn_ref[...] = o_in[...]
    but_own(came_in, recv_o.at[1], heads)
    partial = lax.dot_general(dq_in[...], wbuf[0], over_last, preferred_element_type=f32)
    for s in reversed(range(chunks)):
        chunk = order(s)
        span = cols(chunk * per, per)
        blocks = 2 * per * groups
        own_chunk = at_home & (chunk == my_head // per)
        pl.when(own_chunk)(lambda: came_in(recv_b.at[chunk], blocks - 2))
        pl.when(jnp.logical_not(own_chunk))(lambda: came_in(recv_b.at[chunk], blocks))
        for j in (1, 2):
            if groups == 1:
                summed = dkv_in[j - 1, 0, :, span]
            else:
                summed = dkv_in[j - 1, 0, :, span].astype(f32)
                for i in range(1, groups):
                    summed = summed + dkv_in[j - 1, i, :, span].astype(f32)
                summed = summed.astype(bf)
            partial += lax.dot_general(summed, wbuf[j, :, span], over_last, preferred_element_type=f32)
    for t in range(tp):
        part[t] = partial[:, t * width : (t + 1) * width].astype(bf)
    edge_lo, edge_hi = pl.ds(0, half), pl.ds(rows - half, half)
    def give_back(a, piece, into, peer):
        return [
            remote(piece(t), into.at[mt], send_r.at[a], recv_r.at[a], (peer, t))
            for t in (lax.rem(mt + i, tp) for i in range(1 if a == 2 else 0, tp))
        ]

    @pl.when(has_left)
    def _():
        for copy in give_back(0, lambda t: part.at[t, edge_lo], hi_part, left):
            copy.start()

    @pl.when(has_right)
    def _():
        for copy in give_back(1, lambda t: part.at[t, edge_hi], lo_part, right):
            copy.start()

    for copy in give_back(2, lambda t: part.at[t], own_part, me):
        copy.start()
    own_part[mt] = part[mt]
    target = jnp.where(
        pob < low,
        half - low + pob,
        jnp.where(pob >= count - high, half + rows + pob - (count - high), half + below + pob - low),
    )
    chooser = (target == lax.broadcasted_iota(jnp.int32, (2 * rows, 1), 0)).astype(f32)
    sizes = jnp.maximum(jnp.sum(chooser, axis=1, keepdims=True), 1.0)
    pl.when(has_left)(to_left.wait_send)
    pl.when(has_right)(to_right.wait_send)
    for a in range(2):
        but_own(went_out, send_x.at[a], pairs)
        but_own(went_out, send_x.at[2 + a], heads)
        but_own(went_out, send_h.at[a], heads)
        went_out(send_f.at[a], pairs)

    def handed_over(blocks, spans):
        for b in blocks:
            for i, lo, hi in spans.get(b, ()):
                went_out(send_m.at[i], hi - lo)

    but_own(went_out, send_h.at[2], 2 * pairs, 2)
    for here, plan_of in halves:
        pl.when(here)(functools.partial(handed_over, *plan_of))
    others = own_part.at[pl.ds(0, tp - 1)]
    for here, a, ref in ((has_right, 0, hi_part), (has_left, 1, lo_part)):
        pl.when(here)(lambda: remote(ref, ref, send_r.at[a], recv_r.at[a], mate).wait_recv())
    remote(others, others, send_r.at[2], recv_r.at[2], mate).wait_recv()
    for here, a, ref in ((has_left, 0, hi_part), (has_right, 1, lo_part)):
        pl.when(here)(lambda: remote(ref, ref, send_r.at[a], recv_r.at[a], mate).wait_send())
    remote(others, others, send_r.at[2], recv_r.at[2], mate).wait_send()

    def over_tp(ref):
        value = ref[0].astype(f32)
        for i in range(1, tp):
            value = value + ref[i].astype(f32)
        return value

    returned = jnp.concatenate([over_tp(lo_part), over_tp(own_part), over_tp(hi_part)], axis=0)
    shares = (returned.astype(bf).astype(f32) / sizes).astype(bf)
    grad_ref[...] = lax.dot_general(
        chooser.astype(bf), shares, over_first, preferred_element_type=f32
    ).astype(bf)


def emit_kernel(a_ref, g_ref, a_out, g_out, sem):
    copies = [
        pltpu.make_async_copy(src, dst, sem.at[i]) for i, (src, dst) in enumerate(((a_ref, a_out), (g_ref, g_out)))
    ]
    for copy in copies:
        copy.start()
    for copy in copies:
        copy.wait()


def shards(byte_states, patch_of_byte, patch_first, moved, w_qkv, d_attn):
    n, tp = lax.axis_size("ctx"), lax.axis_size("tp")
    rows, feats = d_attn.shape
    size, model = byte_states.shape
    heads = feats // HD
    pairs = n // 2
    groups = pairs // heads
    total = n * rows
    half = rows // 2
    width = model // tp
    block = per = 2 if heads % 2 == 0 else 1
    steps = heads // block
    assert tp % 2 == 0 and n % 2 == 0 and pairs % heads == 0
    bf, f32, i32 = jnp.bfloat16, jnp.float32, jnp.int32
    dma = pltpu.SemaphoreType.DMA
    results = pl.pallas_call(
        functools.partial(whole_kernel, n, tp, heads, rows, block, per),
        out_shape=[pltpu.VMEM((rows, feats), bf), pltpu.VMEM((size, width), bf)],
        in_specs=[ANY] * 6,
        out_specs=[VM] * 2,
        scratch_shapes=[
            pltpu.VMEM((size, model), bf), pltpu.VMEM((1, size), i32),
            pltpu.SMEM((n,), i32), pltpu.SMEM((2, n), i32),
            pltpu.VMEM(w_qkv.shape, bf), pltpu.VMEM((rows, feats), bf),
            pltpu.VMEM((2, half, model), bf), pltpu.VMEM((2, half, model), bf),
            pltpu.VMEM((rows, model), bf), pltpu.VMEM((3, rows, feats), bf),
            pltpu.VMEM((heads, rows, HD), bf), pltpu.VMEM((heads, rows, HD), bf),
            pltpu.VMEM((pairs, 2, rows, HD), bf), pltpu.VMEM((pairs, 2, rows, HD), bf),
            pltpu.VMEM((steps, block * rows, total), f32),
            pltpu.VMEM((heads, rows, HD), bf), pltpu.VMEM((heads, rows, HD), bf),
            pltpu.VMEM((2, pairs, 2, rows, HD), bf), pltpu.VMEM((2, pairs, rows, HD), bf),
            pltpu.VMEM((total, 2 * HD), f32),
            pltpu.VMEM((rows, feats), bf), pltpu.VMEM((rows, feats), bf),
            pltpu.VMEM((2, groups, rows, feats), bf),
            pltpu.VMEM((tp, rows, width), bf), pltpu.VMEM((tp, rows, width), bf),
            pltpu.VMEM((tp, half, width), bf), pltpu.VMEM((tp, half, width), bf),
            pltpu.VMEM((max(n, per + 2 * per * groups), rows, HD), bf),
            dma((5,)), dma((3,)), dma((2,)), dma((2,)), dma((4,)), dma((4,)), dma((steps,)), dma((2,)), dma((2,)),
            dma((max(2, steps),)), dma((max(2, steps),)), dma((4,)), dma((2,)), dma((heads // per,)), dma((3,)), dma((3,)), pltpu.SemaphoreType.REGULAR((2,)),
        ],
        compiler_params=pltpu.CompilerParams(
            collective_id=0, has_side_effects=True, vmem_limit_bytes=60 << 20
        ),
        name="whole",
    )(byte_states, patch_of_byte.reshape(1, size), patch_first, moved, w_qkv, d_attn)
    results = [pltpu.with_memory_space_constraint(x, pltpu.VMEM) for x in results]
    return tuple(pl.pallas_call(
        emit_kernel,
        out_shape=[jax.ShapeDtypeStruct((rows, feats), bf), jax.ShapeDtypeStruct((size, width), bf)],
        in_specs=[VM, VM],
        out_specs=[ANY] * 2,
        scratch_shapes=[dma((2,))],
        name="emit",
    )(*results))


def solution(mesh):
    placed = (P("ctx", None), P("ctx"), P(), P(), P(None, None, "tp"), P("ctx", "tp"))
    return jax.shard_map(
        shards,
        mesh=mesh,
        in_specs=placed,
        out_specs=(P("ctx", "tp"), P("ctx", "tp")),
        check_vma=False,
    )
```

```python
import functools

import jax
import jax.numpy as jnp
from jax import lax
from jax.experimental import pallas as pl
from jax.experimental.pallas import tpu as pltpu
from jax.sharding import PartitionSpec as P

HD = 128
MESH = pl.DeviceIdType.MESH
VM = pl.BlockSpec(memory_space=pltpu.VMEM)
ANY = pl.BlockSpec(memory_space=pl.ANY)


def remote(src, dst, send, recv, device):
    return pltpu.make_async_remote_copy(
        src_ref=src, dst_ref=dst, send_sem=send, recv_sem=recv, device_id=device, device_id_type=MESH
    )


def each(lo, hi, act):
    def body(i, carry):
        act(i)
        return carry

    lax.fori_loop(lo, hi, body, 0)


def whole_kernel(
    n, tp, heads, rows, block, per,
    bytes_hbm, pob_hbm, first_hbm, moved_hbm, w_hbm, d_hbm,
    attn_ref, grad_ref,
    bytes_ref, pob_ref, first_ref, moved_ref, wbuf, d_ref,
    blk, came, pooled, own3, qb, gb, kb, vb, pa, ob, dqb, dkv, xkv, dkva,
    o_in, dq_in, dkv_in, part, own_part, lo_part, hi_part, tally,
    in_sem, w_sem, send_nb, recv_nb, sent, recv_x, recv_q, recv_f, recv_m, recv_o, recv_b, send_r, recv_r, word,
):
    pairs = n // 2
    groups = pairs // heads
    stride = 2 * groups
    total = n * rows
    half = rows // 2
    scale = HD ** (-0.5)
    bf, f32 = jnp.bfloat16, jnp.float32
    me, mt = lax.axis_index("ctx"), lax.axis_index("tp")
    sub = lax.rem(mt, 2)
    base = mt - sub
    mate = (me, base + 1 - sub)
    parity, place = lax.rem(me, 2), me // 2
    source_tp = base + parity
    at_home = parity == sub
    my_head, my_group = place // groups, lax.rem(place, groups)
    offset = 2 * my_group + sub
    slot = me // stride
    left, right = lax.rem(me + n - 1, n), lax.rem(me + 1, n)
    has_left, has_right = me > 0, me < n - 1
    width = part.shape[2]

    def cols(head, count=1):
        return pl.ds(pl.multiple_of(head * HD, HD), count * HD)

    chunks = heads // per

    def order(s):
        if chunks % 2:
            return lax.rem(my_head // per + (chunks + 1) // 2 + s, chunks)
        here, mid = my_head // per, chunks // 2
        upper = here // mid
        if s < mid:
            return (1 - upper) * (chunks - 1 - s) + upper * s
        back = chunks - 1 - s
        return upper * mid + lax.rem(here + back, mid)

    inputs = [
        pltpu.make_async_copy(src, dst, in_sem.at[i])
        for i, (src, dst) in enumerate((
            (pob_hbm, pob_ref), (first_hbm, first_ref), (moved_hbm, moved_ref), (bytes_hbm, bytes_ref),
            (d_hbm, d_ref),
        ))
    ]
    for copy in inputs:
        copy.start()
    barrier = pltpu.get_barrier_semaphore()

    window = -(-n // 4)

    def greet(i):
        for there, peer in ((me >= i, me - i), (me + i < n, me + i)):
            @pl.when(there)
            def _():
                for core in range(2):
                    pl.semaphore_signal(barrier, inc=1, device_id=(peer, base + core), device_id_type=MESH)

    pl.semaphore_signal(barrier, inc=1, device_id=mate, device_id_type=MESH)
    each(1, window + 1, greet)
    for there, c in ((me >= 0, me), (has_left, me - 1), (has_right, me + 1)):
        for i in range(2, tp):
            pl.when(there)(functools.partial(
                pl.semaphore_signal, barrier, inc=1, device_id=(c, lax.rem(base + i, tp)), device_id_type=MESH
            ))
    beside = has_left.astype(jnp.int32) + has_right.astype(jnp.int32)
    expected = 1 + 2 * (jnp.minimum(me, window) + jnp.minimum(n - 1 - me, window)) + (tp - 2) * (1 + beside)

    def spread(round_):
        far = window << round_
        for there, peer in ((me >= far, me - far), (me + far < n, me + far)):
            pl.when(there)(functools.partial(
                pl.semaphore_signal, word.at[round_], inc=1, device_id=(peer, mt), device_id_type=MESH
            ))

    def heard(round_):
        far = window << round_
        pl.semaphore_wait(word.at[round_], (me >= far).astype(jnp.int32) + (me + far < n).astype(jnp.int32))

    loads = [pltpu.make_async_copy(w_hbm.at[j], wbuf.at[j], w_sem.at[j]) for j in range(3)]
    for copy in inputs[:3]:
        copy.wait()

    def plan(c):
        below = moved_ref[1, lax.rem(c + n - 1, n)]
        above = moved_ref[0, lax.rem(c + 1, n)]
        start = first_ref[c]
        end = jnp.where(c == n - 1, total, first_ref[lax.rem(c + 1, n)])
        return start, end, below, above, moved_ref[0, c], moved_ref[1, c]

    def numbers(c, rank):
        start, end, below, above, low, high = plan(c)
        return jnp.where(
            rank < below,
            start - below + rank,
            jnp.where(rank >= rows - above, end + rank - (rows - above), start + low + rank - below),
        )

    start, end, below, above, low, high = plan(me)
    count = end - start
    rank = lax.broadcasted_iota(jnp.int32, (2 * rows, 1), 0)
    own_rank = rank - 2 * half
    own_local = jnp.where((own_rank >= below) & (own_rank < rows - above), low + own_rank - below, -1)
    up = jnp.where(rank - half < high, count - high + rank - half, -1)
    wanted = jnp.where(rank < half, rank - half + low, jnp.where(rank < 2 * half, up, own_local))
    pob = pob_ref[...]
    member = (pob == wanted).astype(f32)
    lengths = jnp.maximum(jnp.sum(member, axis=1, keepdims=True), 1.0)
    inputs[3].wait()
    for j in (1, 2, 0):
        loads[j].start()
    means = (
        jnp.dot(member.astype(bf), bytes_ref[...], preferred_element_type=f32) / lengths
    ).astype(bf)
    blk[0] = means[:half]
    blk[1] = means[half : 2 * half]

    @pl.when(me == 0)
    def _():
        came[1] = jnp.zeros_like(came[1])
        lo_part[...] = jnp.zeros_like(lo_part)

    @pl.when(me == n - 1)
    def _():
        came[0] = jnp.zeros_like(came[0])
        hi_part[...] = jnp.zeros_like(hi_part)

    pl.semaphore_wait(barrier, expected)
    to_left = remote(blk.at[0], came.at[0], send_nb.at[0], recv_nb.at[0], (left, mt))
    to_right = remote(blk.at[1], came.at[1], send_nb.at[1], recv_nb.at[1], (right, mt))
    pl.when(has_left)(to_left.start)
    pl.when(has_right)(to_right.start)
    spread(0)
    heard(0)
    spread(1)

    def amount(count):
        return tally.at[pl.ds(0, count)]

    def came_in(sem, count):
        remote(amount(count), amount(count), sem, sem, mate).wait_recv()

    def went_out(sem, count):
        remote(amount(count), amount(count), sem, sem, mate).wait_send()

    def but_own(wait, sem, count, own=1):
        pl.when(at_home)(lambda: wait(sem, count - own))
        pl.when(jnp.logical_not(at_home))(lambda: wait(sem, count))

    def start_each(lo, hi, make):
        def act(i):
            other, copy = make(i)
            pl.when(other != me)(copy.start)

        each(lo, hi, act)

    def send_block(a, ref, out):
        def make(i):
            chip = 2 * i + sub
            return chip, remote(
                ref.at[:, cols(i // groups)], out.at[place, parity], sent.at[0], recv_x.at[a],
                (chip, base + parity),
            )

        return make

    def send_query(a, ref, out):
        def make(h):
            chip = 2 * (h * groups + my_group) + sub
            return chip, remote(
                ref.at[:, cols(h)], out.at[slot], sent.at[0],
                recv_q.at[slot // block] if a == 2 else recv_x.at[2], (chip, base + parity),
            )

        return make

    def forward(a, ref):
        return remote(ref.at[:, sub], ref.at[:, sub], sent.at[0], recv_f.at[a], mate)

    def back_query(a, ref, out):
        def make(j):
            c = j * stride + offset
            return c, remote(
                ref.at[j], out.at[:, cols(my_head)], sent.at[0], recv_o.at[a], (c, source_tp)
            )

        return make

    def back_block(i):
        c = 2 * i + sub
        return c, remote(
            dkv.at[:, i, sub], dkv_in.at[:, my_group, :, cols(my_head)], sent.at[0],
            recv_b.at[my_head // per], (c, source_tp),
        )

    send_g, send_q = send_query(3, d_ref, gb), send_query(2, own3.at[0], qb)
    send_k, send_v = send_block(0, own3.at[1], kb), send_block(1, own3.at[2], vb)
    upper = me >= n // 2
    lower = jnp.logical_not(upper)
    early = chunks // 2

    def send_gradients(places):
        for s in places:
            start_each(order(s) * per, order(s) * per + per, send_g)

    @pl.when(upper)
    def _():
        heard(1)
        inputs[4].wait()
        send_gradients(range(early))

    lane = lax.broadcasted_iota(jnp.int32, (1, total), 1)

    def number_keys(c, ids):
        return jnp.where((lane >= c * rows) & (lane < (c + 1) * rows), numbers(c, lane - c * rows), ids)

    kid = lax.fori_loop(0, n, number_keys, jnp.zeros((1, total), jnp.int32))
    pl.when(has_left)(to_right.wait_recv)
    pl.when(has_right)(to_left.wait_recv)
    pooled[pl.ds(0, half)] = means[2 * half : 3 * half] + came[1]
    pooled[pl.ds(half, half)] = means[3 * half :] + came[0]
    mine = cols(my_head)
    makers = (send_q, send_k, send_v)

    def project(kinds):
        for j, places in kinds:
            loads[j].wait()
            for s in places:
                span = cols(order(s) * per, per)
                own3[j, :, span] = jnp.dot(
                    pooled[...], wbuf[j, :, span], preferred_element_type=f32
                ).astype(bf)
                if j == 1 and s == 0:
                    pl.when(lower)(functools.partial(heard, 1))
                each_head = per if j == 0 else per * groups
                start_each(order(s) * each_head, (order(s) + 1) * each_head, makers[j])

    outer = (me < n // 4) | (me >= n - n // 4)
    far_first = list(range(chunks))
    project(((1, far_first), (2, far_first)))
    pl.when(outer)(lambda: project(((0, far_first),)))
    pl.when(jnp.logical_not(outer))(lambda: project(((0, far_first[::-1]),)))

    @pl.when(lower)
    def _():
        inputs[4].wait()
        send_gradients(range(early))

    send_gradients(range(early, chunks))

    @pl.when(parity == sub)
    def _():
        qb[slot] = own3[0, :, mine]
        kb[place, parity] = own3[1, :, mine]
        vb[place, parity] = own3[2, :, mine]
        gb[slot] = d_ref[:, mine]

    over_last = (((1,), (1,)), ((), ()))
    over_first = (((0,), (0,)), ((), ()))
    back_o, back_q = back_query(0, ob, o_in), back_query(1, dqb, dq_in)
    row = lax.broadcasted_iota(jnp.int32, (rows, 1), 0)
    step_keys = max(2, 128 // rows)

    def reach_of(b):
        if b < 0:
            return 0
        reach = min(n, (b + 1) * block * stride + 1)
        return min(n, -(-reach // step_keys) * step_keys)

    def at(c):
        return pl.ds(pl.multiple_of(c * rows, rows), rows)

    def settled_sum(a, c):
        value = dkva[at(c), a * HD : (a + 1) * HD]
        return value * scale if a == 0 else value

    def hand_over(step, lo, hi):
        def act(i):
            for a in range(2):
                dkv[a, i, 1 - sub] = settled_sum(a, 2 * i + 1 - sub).astype(bf)

        each(lo // 2, hi // 2, act)
        span = pl.ds(lo // 2, (hi - lo) // 2)
        remote(dkv.at[:, span, 1 - sub], xkv.at[:, span], sent.at[0], recv_m.at[step], mate).start()

    def send_home(step, lo, hi):
        came_in(recv_m.at[step], hi - lo)

        def act(i):
            for a in range(2):
                dkv[a, i, sub] = (settled_sum(a, 2 * i + sub) + xkv[a, i].astype(f32)).astype(bf)
            other, copy = back_block(i)
            pl.when(other != me)(copy.start)

        each(lo // 2, hi // 2, act)

    steps = list(reversed(range(heads // block)))
    but_own(came_in, recv_x.at[0], pairs)
    forward(0, kb).start()
    but_own(came_in, recv_x.at[1], pairs)
    forward(1, vb).start()
    came_in(recv_f.at[0], pairs)

    def weigh(b):
        lo, reach = b * block, reach_of(b)
        keys = reach * rows
        q = qb[pl.ds(lo, block)].reshape(block * rows, HD)
        k = kb[pl.ds(0, reach // 2)].reshape(keys, HD)
        qid = jnp.concatenate([numbers((lo + j) * stride + offset, row) for j in range(block)], axis=0)
        allowed = qid >= kid[:, :keys]
        score = lax.dot_general(q, k, over_last, preferred_element_type=f32) * scale
        score = jnp.where(allowed, score, -jnp.inf)
        top = jnp.max(score, axis=1, keepdims=True)
        e = jnp.exp(score - top)
        pa[b, :, pl.ds(0, keys)] = e * (1.0 / jnp.sum(e, axis=1, keepdims=True))

    def attend(b):
        lo = b * block
        keys = reach_of(b) * rows
        v = vb[pl.ds(0, reach_of(b) // 2)].reshape(keys, HD)
        out = jnp.dot(pa[b, :, pl.ds(0, keys)].astype(bf), v, preferred_element_type=f32).astype(bf)
        ob[pl.ds(lo, block)] = out.reshape(block, rows, HD)

    def differentiate(b, filled):
        lo = b * block
        keys = reach_of(b) * rows
        q = qb[pl.ds(lo, block)].reshape(block * rows, HD)
        g = gb[pl.ds(lo, block)].reshape(block * rows, HD)
        k = kb[pl.ds(0, reach_of(b) // 2)].reshape(keys, HD)
        v = vb[pl.ds(0, reach_of(b) // 2)].reshape(keys, HD)
        out = ob[pl.ds(lo, block)].reshape(block * rows, HD)
        prob = pa[b, :, pl.ds(0, keys)]
        delta = jnp.sum(g.astype(f32) * out.astype(f32), axis=1, keepdims=True)
        dprob = lax.dot_general(g, v, over_last, preferred_element_type=f32)
        dscore = (prob * (dprob - delta)).astype(bf)
        dq = (jnp.dot(dscore, k, preferred_element_type=f32) * scale).astype(bf)
        dqb[pl.ds(lo, block)] = dq.reshape(block, rows, HD)
        blank = jnp.zeros_like(q)
        both = lax.dot_general(
            jnp.concatenate([dscore, prob.astype(bf)], axis=0),
            jnp.concatenate(
                [jnp.concatenate([q, blank], axis=1), jnp.concatenate([blank, g], axis=1)], axis=0
            ),
            over_first, preferred_element_type=f32,
        )
        old = min(keys, filled)
        if old:
            dkva[pl.ds(0, old)] += both[:old]
        if keys > old:
            dkva[pl.ds(old, keys - old)] = both[old:]
        return max(keys, filled)

    middle = n // 2 // step_keys * step_keys
    whole = [(i, lo, hi) for i, (lo, hi) in enumerate(((0, middle), (middle, n))) if hi > lo]
    falling = (steps, {b: [(b, reach_of(b - 1), reach_of(b))] for b in steps if reach_of(b) > reach_of(b - 1)})
    rising = (steps[::-1], {steps[0]: whole})
    halves = [(upper, rising), (lower, falling)] if len(steps) > 1 else [(me >= 0, falling)]

    def work(blocks, spans):
        lead, first = max(1, len(blocks) // 2), blocks[:1]
        for part_of in (first, blocks[1:]):
            for b in part_of:
                mine_too = at_home & (slot // block == b)
                pl.when(mine_too)(lambda: came_in(recv_q.at[b], block - 1))
                pl.when(jnp.logical_not(mine_too))(lambda: came_in(recv_q.at[b], block))
            for b in part_of:
                weigh(b)
            if part_of is first:
                came_in(recv_f.at[1], pairs)
            for b in part_of:
                attend(b)
            for b in part_of:
                start_each(b * block, (b + 1) * block, back_o)
        but_own(came_in, recv_x.at[2], heads)
        late, filled = [], 0
        for part_of in (blocks[:lead], blocks[lead:]):
            for b in part_of:
                filled = differentiate(b, filled)
            for b in part_of:
                start_each(b * block, (b + 1) * block, back_q)
            ready = [span for b in part_of for span in spans.get(b, ())]
            for span in ready:
                hand_over(*span)
            for span in late:
                send_home(*span)
            late = ready
        for span in late:
            send_home(*span)

    for here, plan_of in halves:
        pl.when(here)(functools.partial(work, *plan_of))

    @pl.when(parity == sub)
    def _():
        o_in[:, mine] = ob[slot]
        dq_in[:, mine] = dqb[slot]
        for a in range(2):
            dkv_in[a, my_group, :, mine] = dkv[a, place, parity]

    but_own(came_in, recv_o.at[0], heads)
    attn_ref[...] = o_in[...]
    but_own(came_in, recv_o.at[1], heads)
    partial = lax.dot_general(dq_in[...], wbuf[0], over_last, preferred_element_type=f32)
    for s in reversed(range(chunks)):
        chunk = order(s)
        span = cols(chunk * per, per)
        blocks = 2 * per * groups
        own_chunk = at_home & (chunk == my_head // per)
        pl.when(own_chunk)(lambda: came_in(recv_b.at[chunk], blocks - 2))
        pl.when(jnp.logical_not(own_chunk))(lambda: came_in(recv_b.at[chunk], blocks))
        for j in (1, 2):
            if groups == 1:
                summed = dkv_in[j - 1, 0, :, span]
            else:
                summed = dkv_in[j - 1, 0, :, span].astype(f32)
                for i in range(1, groups):
                    summed = summed + dkv_in[j - 1, i, :, span].astype(f32)
                summed = summed.astype(bf)
            partial += lax.dot_general(summed, wbuf[j, :, span], over_last, preferred_element_type=f32)
    for t in range(tp):
        part[t] = partial[:, t * width : (t + 1) * width].astype(bf)
    edge_lo, edge_hi = pl.ds(0, half), pl.ds(rows - half, half)
    def give_back(a, piece, into, peer):
        return [
            remote(piece(t), into.at[mt], send_r.at[a], recv_r.at[a], (peer, t))
            for t in (lax.rem(mt + i, tp) for i in range(1 if a == 2 else 0, tp))
        ]

    @pl.when(has_left)
    def _():
        for copy in give_back(0, lambda t: part.at[t, edge_lo], hi_part, left):
            copy.start()

    @pl.when(has_right)
    def _():
        for copy in give_back(1, lambda t: part.at[t, edge_hi], lo_part, right):
            copy.start()

    for copy in give_back(2, lambda t: part.at[t], own_part, me):
        copy.start()
    own_part[mt] = part[mt]
    target = jnp.where(
        pob < low,
        half - low + pob,
        jnp.where(pob >= count - high, half + rows + pob - (count - high), half + below + pob - low),
    )
    chooser = (target == lax.broadcasted_iota(jnp.int32, (2 * rows, 1), 0)).astype(f32)
    sizes = jnp.maximum(jnp.sum(chooser, axis=1, keepdims=True), 1.0)
    pl.when(has_left)(to_left.wait_send)
    pl.when(has_right)(to_right.wait_send)
    but_own(went_out, sent.at[0], 8 * pairs + 4 * heads, 8)
    others = own_part.at[pl.ds(0, tp - 1)]
    for here, a, ref in ((has_right, 0, hi_part), (has_left, 1, lo_part)):
        pl.when(here)(lambda: remote(ref, ref, send_r.at[a], recv_r.at[a], mate).wait_recv())
    remote(others, others, send_r.at[2], recv_r.at[2], mate).wait_recv()
    for here, a, ref in ((has_left, 0, hi_part), (has_right, 1, lo_part)):
        pl.when(here)(lambda: remote(ref, ref, send_r.at[a], recv_r.at[a], mate).wait_send())
    remote(others, others, send_r.at[2], recv_r.at[2], mate).wait_send()

    def over_tp(ref):
        value = ref[0].astype(f32)
        for i in range(1, tp):
            value = value + ref[i].astype(f32)
        return value

    returned = jnp.concatenate([over_tp(lo_part), over_tp(own_part), over_tp(hi_part)], axis=0)
    shares = (returned.astype(bf).astype(f32) / sizes).astype(bf)
    grad_ref[...] = lax.dot_general(
        chooser.astype(bf), shares, over_first, preferred_element_type=f32
    ).astype(bf)


def emit_kernel(a_ref, g_ref, a_out, g_out, sem):
    copies = [
        pltpu.make_async_copy(src, dst, sem.at[i]) for i, (src, dst) in enumerate(((a_ref, a_out), (g_ref, g_out)))
    ]
    for copy in copies:
        copy.start()
    for copy in copies:
        copy.wait()


def shards(byte_states, patch_of_byte, patch_first, moved, w_qkv, d_attn):
    n, tp = lax.axis_size("ctx"), lax.axis_size("tp")
    rows, feats = d_attn.shape
    size, model = byte_states.shape
    heads = feats // HD
    pairs = n // 2
    groups = pairs // heads
    total = n * rows
    half = rows // 2
    width = model // tp
    block = per = 2 if heads % 2 == 0 else 1
    steps = heads // block
    assert tp % 2 == 0 and n % 2 == 0 and pairs % heads == 0
    bf, f32, i32 = jnp.bfloat16, jnp.float32, jnp.int32
    dma = pltpu.SemaphoreType.DMA
    results = pl.pallas_call(
        functools.partial(whole_kernel, n, tp, heads, rows, block, per),
        out_shape=[pltpu.VMEM((rows, feats), bf), pltpu.VMEM((size, width), bf)],
        in_specs=[ANY] * 6,
        out_specs=[VM] * 2,
        scratch_shapes=[
            pltpu.VMEM((size, model), bf), pltpu.VMEM((1, size), i32),
            pltpu.SMEM((n,), i32), pltpu.SMEM((2, n), i32),
            pltpu.VMEM(w_qkv.shape, bf), pltpu.VMEM((rows, feats), bf),
            pltpu.VMEM((2, half, model), bf), pltpu.VMEM((2, half, model), bf),
            pltpu.VMEM((rows, model), bf), pltpu.VMEM((3, rows, feats), bf),
            pltpu.VMEM((heads, rows, HD), bf), pltpu.VMEM((heads, rows, HD), bf),
            pltpu.VMEM((pairs, 2, rows, HD), bf), pltpu.VMEM((pairs, 2, rows, HD), bf),
            pltpu.VMEM((steps, block * rows, total), f32),
            pltpu.VMEM((heads, rows, HD), bf), pltpu.VMEM((heads, rows, HD), bf),
            pltpu.VMEM((2, pairs, 2, rows, HD), bf), pltpu.VMEM((2, pairs, rows, HD), bf),
            pltpu.VMEM((total, 2 * HD), f32),
            pltpu.VMEM((rows, feats), bf), pltpu.VMEM((rows, feats), bf),
            pltpu.VMEM((2, groups, rows, feats), bf),
            pltpu.VMEM((tp, rows, width), bf), pltpu.VMEM((tp, rows, width), bf),
            pltpu.VMEM((tp, half, width), bf), pltpu.VMEM((tp, half, width), bf),
            pltpu.VMEM((8 * pairs + 4 * heads, rows, HD), bf),
            dma((5,)), dma((3,)), dma((2,)), dma((2,)), dma((1,)), dma((3,)), dma((steps,)), dma((2,)),
            dma((max(2, steps),)), dma((2,)), dma((heads // per,)), dma((3,)), dma((3,)),
            pltpu.SemaphoreType.REGULAR((2,)),
        ],
        compiler_params=pltpu.CompilerParams(
            collective_id=0, has_side_effects=True, vmem_limit_bytes=60 << 20
        ),
        name="whole",
    )(byte_states, patch_of_byte.reshape(1, size), patch_first, moved, w_qkv, d_attn)
    results = [pltpu.with_memory_space_constraint(x, pltpu.VMEM) for x in results]
    return tuple(pl.pallas_call(
        emit_kernel,
        out_shape=[jax.ShapeDtypeStruct((rows, feats), bf), jax.ShapeDtypeStruct((size, width), bf)],
        in_specs=[VM, VM],
        out_specs=[ANY] * 2,
        scratch_shapes=[dma((2,))],
        name="emit",
    )(*results))


def solution(mesh):
    placed = (P("ctx", None), P("ctx"), P(), P(), P(None, None, "tp"), P("ctx", "tp"))
    return jax.shard_map(
        shards,
        mesh=mesh,
        in_specs=placed,
        out_specs=(P("ctx", "tp"), P("ctx", "tp")),
        check_vma=False,
    )
```

```python
import functools

import jax
import jax.numpy as jnp
from jax import lax
from jax.experimental import pallas as pl
from jax.experimental.pallas import tpu as pltpu
from jax.sharding import PartitionSpec as P

HD = 128
MESH = pl.DeviceIdType.MESH
VM = pl.BlockSpec(memory_space=pltpu.VMEM)
ANY = pl.BlockSpec(memory_space=pl.ANY)


def remote(src, dst, send, recv, device):
    return pltpu.make_async_remote_copy(
        src_ref=src, dst_ref=dst, send_sem=send, recv_sem=recv, device_id=device, device_id_type=MESH
    )


def each(lo, hi, act):
    def body(i, carry):
        act(i)
        return carry

    lax.fori_loop(lo, hi, body, 0)


def whole_kernel(
    n, tp, heads, rows, block, per,
    bytes_hbm, pob_hbm, first_hbm, moved_hbm, w_hbm, d_hbm,
    attn_ref, grad_ref,
    bytes_ref, pob_ref, first_ref, moved_ref, wbuf, d_ref,
    blk, came, pooled, own3, qb, gb, kb, vb, pa, ob, dqb, dkv, xkv, dkva, wt,
    o_in, dq_in, dkv_in, part, own_part, lo_part, hi_part, tally,
    in_sem, w_sem, send_nb, recv_nb, sent, recv_x, recv_q, recv_f, recv_m, recv_o, recv_b, send_r, recv_r, word,
):
    pairs = n // 2
    groups = pairs // heads
    stride = 2 * groups
    total = n * rows
    half = rows // 2
    scale = HD ** (-0.5)
    bf, f32 = jnp.bfloat16, jnp.float32
    me, mt = lax.axis_index("ctx"), lax.axis_index("tp")
    sub = lax.rem(mt, 2)
    base = mt - sub
    mate = (me, base + 1 - sub)
    parity, place = lax.rem(me, 2), me // 2
    source_tp = base + parity
    at_home = parity == sub
    my_head, my_group = place // groups, lax.rem(place, groups)
    offset = 2 * my_group + sub
    slot = me // stride
    left, right = lax.rem(me + n - 1, n), lax.rem(me + 1, n)
    has_left, has_right = me > 0, me < n - 1
    width = part.shape[2]

    def cols(head, count=1):
        return pl.ds(pl.multiple_of(head * HD, HD), count * HD)

    chunks = heads // per

    def order(s):
        if chunks % 2:
            return lax.rem(my_head // per + (chunks + 1) // 2 + s, chunks)
        here, mid = my_head // per, chunks // 2
        upper = here // mid
        if s < mid:
            return (1 - upper) * (chunks - 1 - s) + upper * s
        back = chunks - 1 - s
        return upper * mid + lax.rem(here + back, mid)

    inputs = [
        pltpu.make_async_copy(src, dst, in_sem.at[i])
        for i, (src, dst) in enumerate((
            (pob_hbm, pob_ref), (first_hbm, first_ref), (moved_hbm, moved_ref), (bytes_hbm, bytes_ref),
            (d_hbm, d_ref),
        ))
    ]
    for copy in inputs:
        copy.start()
    barrier = pltpu.get_barrier_semaphore()

    window = -(-n // 4)

    def greet(i):
        for there, peer in ((me >= i, me - i), (me + i < n, me + i)):
            @pl.when(there)
            def _():
                for core in range(2):
                    pl.semaphore_signal(barrier, inc=1, device_id=(peer, base + core), device_id_type=MESH)

    pl.semaphore_signal(barrier, inc=1, device_id=mate, device_id_type=MESH)
    each(1, window + 1, greet)
    for there, c in ((me >= 0, me), (has_left, me - 1), (has_right, me + 1)):
        for i in range(2, tp):
            pl.when(there)(functools.partial(
                pl.semaphore_signal, barrier, inc=1, device_id=(c, lax.rem(base + i, tp)), device_id_type=MESH
            ))
    beside = has_left.astype(jnp.int32) + has_right.astype(jnp.int32)
    expected = 1 + 2 * (jnp.minimum(me, window) + jnp.minimum(n - 1 - me, window)) + (tp - 2) * (1 + beside)

    def spread(round_):
        far = window << round_
        for there, peer in ((me >= far, me - far), (me + far < n, me + far)):
            pl.when(there)(functools.partial(
                pl.semaphore_signal, word.at[round_], inc=1, device_id=(peer, mt), device_id_type=MESH
            ))

    def heard(round_):
        far = window << round_
        pl.semaphore_wait(word.at[round_], (me >= far).astype(jnp.int32) + (me + far < n).astype(jnp.int32))

    loads = [pltpu.make_async_copy(w_hbm.at[j], wbuf.at[j], w_sem.at[j]) for j in range(3)]
    for copy in inputs[:3]:
        copy.wait()

    def plan(c):
        below = moved_ref[1, lax.rem(c + n - 1, n)]
        above = moved_ref[0, lax.rem(c + 1, n)]
        start = first_ref[c]
        end = jnp.where(c == n - 1, total, first_ref[lax.rem(c + 1, n)])
        return start, end, below, above, moved_ref[0, c], moved_ref[1, c]

    def numbers(c, rank):
        start, end, below, above, low, high = plan(c)
        return jnp.where(
            rank < below,
            start - below + rank,
            jnp.where(rank >= rows - above, end + rank - (rows - above), start + low + rank - below),
        )

    start, end, below, above, low, high = plan(me)
    count = end - start
    rank = lax.broadcasted_iota(jnp.int32, (2 * rows, 1), 0)
    own_rank = rank - 2 * half
    own_local = jnp.where((own_rank >= below) & (own_rank < rows - above), low + own_rank - below, -1)
    up = jnp.where(rank - half < high, count - high + rank - half, -1)
    wanted = jnp.where(rank < half, rank - half + low, jnp.where(rank < 2 * half, up, own_local))
    pob = pob_ref[...]
    member = (pob == wanted).astype(f32)
    lengths = jnp.maximum(jnp.sum(member, axis=1, keepdims=True), 1.0)
    inputs[3].wait()
    for j in (1, 2, 0):
        loads[j].start()
    means = (
        jnp.dot(member.astype(bf), bytes_ref[...], preferred_element_type=f32) / lengths
    ).astype(bf)
    blk[0] = means[:half]
    blk[1] = means[half : 2 * half]

    @pl.when(me == 0)
    def _():
        came[1] = jnp.zeros_like(came[1])
        lo_part[...] = jnp.zeros_like(lo_part)

    @pl.when(me == n - 1)
    def _():
        came[0] = jnp.zeros_like(came[0])
        hi_part[...] = jnp.zeros_like(hi_part)

    pl.semaphore_wait(barrier, expected)
    to_left = remote(blk.at[0], came.at[0], send_nb.at[0], recv_nb.at[0], (left, mt))
    to_right = remote(blk.at[1], came.at[1], send_nb.at[1], recv_nb.at[1], (right, mt))
    pl.when(has_left)(to_left.start)
    pl.when(has_right)(to_right.start)
    spread(0)
    heard(0)
    spread(1)

    def amount(count):
        return tally.at[pl.ds(0, count)]

    def came_in(sem, count):
        remote(amount(count), amount(count), sem, sem, mate).wait_recv()

    def went_out(sem, count):
        remote(amount(count), amount(count), sem, sem, mate).wait_send()

    def but_own(wait, sem, count, own=1):
        pl.when(at_home)(lambda: wait(sem, count - own))
        pl.when(jnp.logical_not(at_home))(lambda: wait(sem, count))

    def start_each(lo, hi, make):
        def act(i):
            other, copy = make(i)
            pl.when(other != me)(copy.start)

        each(lo, hi, act)

    def send_block(a, ref, out):
        def make(i):
            chip = 2 * i + sub
            return chip, remote(
                ref.at[:, cols(i // groups)], out.at[place, parity], sent.at[0], recv_x.at[a],
                (chip, base + parity),
            )

        return make

    def send_query(a, ref, out):
        def make(h):
            chip = 2 * (h * groups + my_group) + sub
            return chip, remote(
                ref.at[:, cols(h)], out.at[slot], sent.at[0],
                recv_q.at[slot // block] if a == 2 else recv_x.at[2], (chip, base + parity),
            )

        return make

    def forward(a, ref):
        return remote(ref.at[:, sub], ref.at[:, sub], sent.at[0], recv_f.at[a], mate)

    def back_query(a, ref, out):
        def make(j):
            c = j * stride + offset
            return c, remote(
                ref.at[j], out.at[:, cols(my_head)], sent.at[0], recv_o.at[a], (c, source_tp)
            )

        return make

    def back_block(i):
        c = 2 * i + sub
        return c, remote(
            dkv.at[:, i, sub], dkv_in.at[:, my_group, :, cols(my_head)], sent.at[0],
            recv_b.at[my_head // per], (c, source_tp),
        )

    send_g, send_q = send_query(3, d_ref, gb), send_query(2, own3.at[0], qb)
    send_k, send_v = send_block(0, own3.at[1], kb), send_block(1, own3.at[2], vb)
    upper = me >= n // 2
    lower = jnp.logical_not(upper)
    early = chunks // 2

    def send_gradients(places):
        for s in places:
            start_each(order(s) * per, order(s) * per + per, send_g)

    @pl.when(upper)
    def _():
        heard(1)
        inputs[4].wait()
        send_gradients(range(early))

    lane = lax.broadcasted_iota(jnp.int32, (1, total), 1)

    def number_keys(c, ids):
        return jnp.where((lane >= c * rows) & (lane < (c + 1) * rows), numbers(c, lane - c * rows), ids)

    kid = lax.fori_loop(0, n, number_keys, jnp.zeros((1, total), jnp.int32))
    pl.when(has_left)(to_right.wait_recv)
    pl.when(has_right)(to_left.wait_recv)
    pooled[pl.ds(0, half)] = means[2 * half : 3 * half] + came[1]
    pooled[pl.ds(half, half)] = means[3 * half :] + came[0]
    mine = cols(my_head)
    makers = (send_q, send_k, send_v)

    for j in (1, 2, 0):
        loads[j].wait()

    def project(kinds):
        for j, places in kinds:
            for s in places:
                span = cols(order(s) * per, per)
                own3[j, :, span] = jnp.dot(
                    pooled[...], wbuf[j, :, span], preferred_element_type=f32
                ).astype(bf)
                if j == 1 and s == 0:
                    pl.when(lower)(functools.partial(heard, 1))
                each_head = per if j == 0 else per * groups
                start_each(order(s) * each_head, (order(s) + 1) * each_head, makers[j])

    outer = (me < n // 4) | (me >= n - n // 4)
    far_first = list(range(chunks))
    distant, close = far_first[:early], far_first[early:]
    project(((1, distant), (2, distant)))
    pl.when(outer)(lambda: project(((0, distant), (1, close), (2, close), (0, close))))
    pl.when(jnp.logical_not(outer))(lambda: project(((1, close), (2, close), (0, close), (0, distant))))

    @pl.when(lower)
    def _():
        inputs[4].wait()
        send_gradients(range(early))

    send_gradients(range(early, chunks))

    @pl.when(parity == sub)
    def _():
        qb[slot] = own3[0, :, mine]
        kb[place, parity] = own3[1, :, mine]
        vb[place, parity] = own3[2, :, mine]
        gb[slot] = d_ref[:, mine]

    over_last = (((1,), (1,)), ((), ()))
    over_first = (((0,), (0,)), ((), ()))
    back_o, back_q = back_query(0, ob, o_in), back_query(1, dqb, dq_in)
    row = lax.broadcasted_iota(jnp.int32, (rows, 1), 0)
    step_keys = max(2, 128 // rows)

    def reach_of(b):
        if b < 0:
            return 0
        reach = min(n, (b + 1) * block * stride + 1)
        return min(n, -(-reach // step_keys) * step_keys)

    def at(c):
        return pl.ds(pl.multiple_of(c * rows, rows), rows)

    def settled_sum(a, c):
        value = dkva[at(c), a * HD : (a + 1) * HD]
        return value * scale if a == 0 else value

    def hand_over(step, lo, hi):
        def act(i):
            for a in range(2):
                dkv[a, i, 1 - sub] = settled_sum(a, 2 * i + 1 - sub).astype(bf)

        each(lo // 2, hi // 2, act)
        span = pl.ds(lo // 2, (hi - lo) // 2)
        remote(dkv.at[:, span, 1 - sub], xkv.at[:, span], sent.at[0], recv_m.at[step], mate).start()

    def send_home(step, lo, hi):
        came_in(recv_m.at[step], hi - lo)

        def act(i):
            for a in range(2):
                dkv[a, i, sub] = (settled_sum(a, 2 * i + sub) + xkv[a, i].astype(f32)).astype(bf)
            other, copy = back_block(i)
            pl.when(other != me)(copy.start)

        each(lo // 2, hi // 2, act)

    steps = list(reversed(range(heads // block)))
    but_own(came_in, recv_x.at[0], pairs)
    forward(0, kb).start()
    for j in (1, 2):
        wt[j - 1] = wbuf[j].T
    but_own(came_in, recv_x.at[1], pairs)
    forward(1, vb).start()
    came_in(recv_f.at[0], pairs)

    def weigh(b):
        lo, reach = b * block, reach_of(b)
        keys = reach * rows
        q = qb[pl.ds(lo, block)].reshape(block * rows, HD)
        k = kb[pl.ds(0, reach // 2)].reshape(keys, HD)
        qid = jnp.concatenate([numbers((lo + j) * stride + offset, row) for j in range(block)], axis=0)
        allowed = qid >= kid[:, :keys]
        score = lax.dot_general(q, k, over_last, preferred_element_type=f32) * scale
        score = jnp.where(allowed, score, -jnp.inf)
        top = jnp.max(score, axis=1, keepdims=True)
        e = jnp.exp(score - top)
        pa[b, :, pl.ds(0, keys)] = e * (1.0 / jnp.sum(e, axis=1, keepdims=True))

    def attend(b):
        lo = b * block
        keys = reach_of(b) * rows
        v = vb[pl.ds(0, reach_of(b) // 2)].reshape(keys, HD)
        out = jnp.dot(pa[b, :, pl.ds(0, keys)].astype(bf), v, preferred_element_type=f32).astype(bf)
        ob[pl.ds(lo, block)] = out.reshape(block, rows, HD)

    def differentiate(b, filled):
        lo = b * block
        keys = reach_of(b) * rows
        q = qb[pl.ds(lo, block)].reshape(block * rows, HD)
        g = gb[pl.ds(lo, block)].reshape(block * rows, HD)
        k = kb[pl.ds(0, reach_of(b) // 2)].reshape(keys, HD)
        v = vb[pl.ds(0, reach_of(b) // 2)].reshape(keys, HD)
        out = ob[pl.ds(lo, block)].reshape(block * rows, HD)
        prob = pa[b, :, pl.ds(0, keys)]
        delta = jnp.sum(g.astype(f32) * out.astype(f32), axis=1, keepdims=True)
        dprob = lax.dot_general(g, v, over_last, preferred_element_type=f32)
        dscore = (prob * (dprob - delta)).astype(bf)
        dq = (jnp.dot(dscore, k, preferred_element_type=f32) * scale).astype(bf)
        dqb[pl.ds(lo, block)] = dq.reshape(block, rows, HD)
        blank = jnp.zeros_like(q)
        both = lax.dot_general(
            jnp.concatenate([dscore, prob.astype(bf)], axis=0),
            jnp.concatenate(
                [jnp.concatenate([q, blank], axis=1), jnp.concatenate([blank, g], axis=1)], axis=0
            ),
            over_first, preferred_element_type=f32,
        )
        old = min(keys, filled)
        if old:
            dkva[pl.ds(0, old)] += both[:old]
        if keys > old:
            dkva[pl.ds(old, keys - old)] = both[old:]
        return max(keys, filled)

    middle = n // 2 // step_keys * step_keys
    whole = [(i, lo, hi) for i, (lo, hi) in enumerate(((0, middle), (middle, n))) if hi > lo]
    falling = (steps, {b: [(b, reach_of(b - 1), reach_of(b))] for b in steps if reach_of(b) > reach_of(b - 1)})
    rising = (steps[::-1], {steps[0]: whole})
    halves = [(upper, rising), (lower, falling)] if len(steps) > 1 else [(me >= 0, falling)]

    def work(blocks, spans):
        lead, first = max(1, len(blocks) // 2), blocks[:1]
        for part_of in (first, blocks[1:]):
            for b in part_of:
                mine_too = at_home & (slot // block == b)
                pl.when(mine_too)(lambda: came_in(recv_q.at[b], block - 1))
                pl.when(jnp.logical_not(mine_too))(lambda: came_in(recv_q.at[b], block))
            for b in part_of:
                weigh(b)
            if part_of is first:
                came_in(recv_f.at[1], pairs)
            for b in part_of:
                attend(b)
            for b in part_of:
                start_each(b * block, (b + 1) * block, back_o)
        but_own(came_in, recv_x.at[2], heads)
        late, filled = [], 0
        for part_of in (blocks[:lead], blocks[lead:]):
            for b in part_of:
                filled = differentiate(b, filled)
            for b in part_of:
                start_each(b * block, (b + 1) * block, back_q)
            ready = [span for b in part_of for span in spans.get(b, ())]
            for span in ready:
                hand_over(*span)
            for span in late:
                send_home(*span)
            late = ready
        for span in late:
            send_home(*span)

    for here, plan_of in halves:
        pl.when(here)(functools.partial(work, *plan_of))

    @pl.when(parity == sub)
    def _():
        o_in[:, mine] = ob[slot]
        dq_in[:, mine] = dqb[slot]
        for a in range(2):
            dkv_in[a, my_group, :, mine] = dkv[a, place, parity]

    but_own(came_in, recv_o.at[0], heads)
    attn_ref[...] = o_in[...]
    but_own(came_in, recv_o.at[1], heads)
    partial = lax.dot_general(dq_in[...], wbuf[0], over_last, preferred_element_type=f32)
    for s in reversed(range(chunks)):
        chunk = order(s)
        span = cols(chunk * per, per)
        blocks = 2 * per * groups
        own_chunk = at_home & (chunk == my_head // per)
        pl.when(own_chunk)(lambda: came_in(recv_b.at[chunk], blocks - 2))
        pl.when(jnp.logical_not(own_chunk))(lambda: came_in(recv_b.at[chunk], blocks))
        for j in (1, 2):
            if groups == 1:
                summed = dkv_in[j - 1, 0, :, span]
            else:
                summed = dkv_in[j - 1, 0, :, span].astype(f32)
                for i in range(1, groups):
                    summed = summed + dkv_in[j - 1, i, :, span].astype(f32)
                summed = summed.astype(bf)
            partial += jnp.dot(summed, wt[j - 1, span], preferred_element_type=f32)
    for t in range(tp):
        part[t] = partial[:, t * width : (t + 1) * width].astype(bf)
    edge_lo, edge_hi = pl.ds(0, half), pl.ds(rows - half, half)
    def give_back(a, piece, into, peer):
        return [
            remote(piece(t), into.at[mt], send_r.at[a], recv_r.at[a], (peer, t))
            for t in (lax.rem(mt + i, tp) for i in range(1 if a == 2 else 0, tp))
        ]

    @pl.when(has_left)
    def _():
        for copy in give_back(0, lambda t: part.at[t, edge_lo], hi_part, left):
            copy.start()

    @pl.when(has_right)
    def _():
        for copy in give_back(1, lambda t: part.at[t, edge_hi], lo_part, right):
            copy.start()

    for copy in give_back(2, lambda t: part.at[t], own_part, me):
        copy.start()
    own_part[mt] = part[mt]
    target = jnp.where(
        pob < low,
        half - low + pob,
        jnp.where(pob >= count - high, half + rows + pob - (count - high), half + below + pob - low),
    )
    chooser = (target == lax.broadcasted_iota(jnp.int32, (2 * rows, 1), 0)).astype(f32)
    sizes = jnp.maximum(jnp.sum(chooser, axis=1, keepdims=True), 1.0)
    pl.when(has_left)(to_left.wait_send)
    pl.when(has_right)(to_right.wait_send)
    but_own(went_out, sent.at[0], 8 * pairs + 4 * heads, 8)
    others = own_part.at[pl.ds(0, tp - 1)]
    for here, a, ref in ((has_right, 0, hi_part), (has_left, 1, lo_part)):
        pl.when(here)(lambda: remote(ref, ref, send_r.at[a], recv_r.at[a], mate).wait_recv())
    remote(others, others, send_r.at[2], recv_r.at[2], mate).wait_recv()
    for here, a, ref in ((has_left, 0, hi_part), (has_right, 1, lo_part)):
        pl.when(here)(lambda: remote(ref, ref, send_r.at[a], recv_r.at[a], mate).wait_send())
    remote(others, others, send_r.at[2], recv_r.at[2], mate).wait_send()

    def over_tp(ref):
        value = ref[0].astype(f32)
        for i in range(1, tp):
            value = value + ref[i].astype(f32)
        return value

    returned = jnp.concatenate([over_tp(lo_part), over_tp(own_part), over_tp(hi_part)], axis=0)
    shares = (returned.astype(bf).astype(f32) / sizes).astype(bf)
    grad_ref[...] = lax.dot_general(
        chooser.astype(bf), shares, over_first, preferred_element_type=f32
    ).astype(bf)


def emit_kernel(a_ref, g_ref, a_out, g_out, sem):
    copies = [
        pltpu.make_async_copy(src, dst, sem.at[i]) for i, (src, dst) in enumerate(((a_ref, a_out), (g_ref, g_out)))
    ]
    for copy in copies:
        copy.start()
    for copy in copies:
        copy.wait()


def shards(byte_states, patch_of_byte, patch_first, moved, w_qkv, d_attn):
    n, tp = lax.axis_size("ctx"), lax.axis_size("tp")
    rows, feats = d_attn.shape
    size, model = byte_states.shape
    heads = feats // HD
    pairs = n // 2
    groups = pairs // heads
    total = n * rows
    half = rows // 2
    width = model // tp
    block = per = 2 if heads % 2 == 0 else 1
    steps = heads // block
    assert tp % 2 == 0 and n % 2 == 0 and pairs % heads == 0
    bf, f32, i32 = jnp.bfloat16, jnp.float32, jnp.int32
    dma = pltpu.SemaphoreType.DMA
    results = pl.pallas_call(
        functools.partial(whole_kernel, n, tp, heads, rows, block, per),
        out_shape=[pltpu.VMEM((rows, feats), bf), pltpu.VMEM((size, width), bf)],
        in_specs=[ANY] * 6,
        out_specs=[VM] * 2,
        scratch_shapes=[
            pltpu.VMEM((size, model), bf), pltpu.VMEM((1, size), i32),
            pltpu.SMEM((n,), i32), pltpu.SMEM((2, n), i32),
            pltpu.VMEM(w_qkv.shape, bf), pltpu.VMEM((rows, feats), bf),
            pltpu.VMEM((2, half, model), bf), pltpu.VMEM((2, half, model), bf),
            pltpu.VMEM((rows, model), bf), pltpu.VMEM((3, rows, feats), bf),
            pltpu.VMEM((heads, rows, HD), bf), pltpu.VMEM((heads, rows, HD), bf),
            pltpu.VMEM((pairs, 2, rows, HD), bf), pltpu.VMEM((pairs, 2, rows, HD), bf),
            pltpu.VMEM((steps, block * rows, total), f32),
            pltpu.VMEM((heads, rows, HD), bf), pltpu.VMEM((heads, rows, HD), bf),
            pltpu.VMEM((2, pairs, 2, rows, HD), bf), pltpu.VMEM((2, pairs, rows, HD), bf),
            pltpu.VMEM((total, 2 * HD), f32), pltpu.VMEM((2, feats, model), bf),
            pltpu.VMEM((rows, feats), bf), pltpu.VMEM((rows, feats), bf),
            pltpu.VMEM((2, groups, rows, feats), bf),
            pltpu.VMEM((tp, rows, width), bf), pltpu.VMEM((tp, rows, width), bf),
            pltpu.VMEM((tp, half, width), bf), pltpu.VMEM((tp, half, width), bf),
            pltpu.VMEM((8 * pairs + 4 * heads, rows, HD), bf),
            dma((5,)), dma((3,)), dma((2,)), dma((2,)), dma((1,)), dma((3,)), dma((steps,)), dma((2,)),
            dma((max(2, steps),)), dma((2,)), dma((heads // per,)), dma((3,)), dma((3,)),
            pltpu.SemaphoreType.REGULAR((2,)),
        ],
        compiler_params=pltpu.CompilerParams(
            collective_id=0, has_side_effects=True, vmem_limit_bytes=60 << 20
        ),
        name="whole",
    )(byte_states, patch_of_byte.reshape(1, size), patch_first, moved, w_qkv, d_attn)
    results = [pltpu.with_memory_space_constraint(x, pltpu.VMEM) for x in results]
    return tuple(pl.pallas_call(
        emit_kernel,
        out_shape=[jax.ShapeDtypeStruct((rows, feats), bf), jax.ShapeDtypeStruct((size, width), bf)],
        in_specs=[VM, VM],
        out_specs=[ANY] * 2,
        scratch_shapes=[dma((2,))],
        name="emit",
    )(*results))


def solution(mesh):
    placed = (P("ctx", None), P("ctx"), P(), P(), P(None, None, "tp"), P("ctx", "tp"))
    return jax.shard_map(
        shards,
        mesh=mesh,
        in_specs=placed,
        out_specs=(P("ctx", "tp"), P("ctx", "tp")),
        check_vma=False,
    )
```

```python
import functools

import jax
import jax.numpy as jnp
from jax import lax
from jax.experimental import pallas as pl
from jax.experimental.pallas import tpu as pltpu
from jax.sharding import PartitionSpec as P

HD = 128
MESH = pl.DeviceIdType.MESH
VM = pl.BlockSpec(memory_space=pltpu.VMEM)
ANY = pl.BlockSpec(memory_space=pl.ANY)


def remote(src, dst, send, recv, device):
    return pltpu.make_async_remote_copy(
        src_ref=src, dst_ref=dst, send_sem=send, recv_sem=recv, device_id=device, device_id_type=MESH
    )


def each(lo, hi, act):
    def body(i, carry):
        act(i)
        return carry

    lax.fori_loop(lo, hi, body, 0)


def whole_kernel(
    n, tp, heads, rows, block, per,
    bytes_hbm, pob_hbm, first_hbm, moved_hbm, w_hbm, d_hbm,
    attn_ref, grad_ref,
    bytes_ref, pob_ref, first_ref, moved_ref, wbuf, d_ref,
    blk, came, pooled, own3, qb, gb, kb, vb, pa, ob, dqb, dkv, xkv, dkva, wt,
    o_in, dq_in, dkv_in, part, own_part, lo_part, hi_part, tally,
    in_sem, w_sem, send_nb, recv_nb, sent, recv_x, recv_q, recv_f, recv_m, recv_o, recv_b, send_r, recv_r, word,
):
    pairs = n // 2
    groups = pairs // heads
    stride = 2 * groups
    total = n * rows
    half = rows // 2
    scale = HD ** (-0.5)
    bf, f32 = jnp.bfloat16, jnp.float32
    me, mt = lax.axis_index("ctx"), lax.axis_index("tp")
    sub = lax.rem(mt, 2)
    base = mt - sub
    mate = (me, base + 1 - sub)
    parity, place = lax.rem(me, 2), me // 2
    source_tp = base + parity
    at_home = parity == sub
    my_head, my_group = place // groups, lax.rem(place, groups)
    offset = 2 * my_group + sub
    slot = me // stride
    left, right = lax.rem(me + n - 1, n), lax.rem(me + 1, n)
    has_left, has_right = me > 0, me < n - 1
    width = part.shape[2]

    def cols(head, count=1):
        return pl.ds(pl.multiple_of(head * HD, HD), count * HD)

    chunks = heads // per

    def order(s):
        if chunks % 2:
            return lax.rem(my_head // per + (chunks + 1) // 2 + s, chunks)
        here, mid = my_head // per, chunks // 2
        upper = here // mid
        if s < mid:
            return (1 - upper) * (chunks - 1 - s) + upper * s
        back = chunks - 1 - s
        return upper * mid + lax.rem(here + back, mid)

    size = bytes_ref.shape[0]
    pieces = 4 if size % 64 == 0 else 1
    for i in range(pieces):
        piece = pl.ds(i * (size // pieces), size // pieces)
        pltpu.make_async_copy(bytes_hbm.at[piece], bytes_ref.at[piece], in_sem.at[3]).start()
    inputs = [
        pltpu.make_async_copy(src, dst, in_sem.at[i])
        for i, (src, dst) in enumerate((
            (pob_hbm, pob_ref), (first_hbm, first_ref), (moved_hbm, moved_ref), (bytes_hbm, bytes_ref),
            (d_hbm, d_ref),
        ))
    ]
    for copy in inputs[:3] + inputs[4:]:
        copy.start()
    barrier = pltpu.get_barrier_semaphore()

    window = -(-n // 4)

    def greet(i):
        for there, peer in ((me >= i, me - i), (me + i < n, me + i)):
            @pl.when(there)
            def _():
                for core in range(2):
                    pl.semaphore_signal(barrier, inc=1, device_id=(peer, base + core), device_id_type=MESH)

    pl.semaphore_signal(barrier, inc=1, device_id=mate, device_id_type=MESH)
    each(1, window + 1, greet)
    for there, c in ((me >= 0, me), (has_left, me - 1), (has_right, me + 1)):
        for i in range(2, tp):
            pl.when(there)(functools.partial(
                pl.semaphore_signal, barrier, inc=1, device_id=(c, lax.rem(base + i, tp)), device_id_type=MESH
            ))
    beside = has_left.astype(jnp.int32) + has_right.astype(jnp.int32)
    expected = 1 + 2 * (jnp.minimum(me, window) + jnp.minimum(n - 1 - me, window)) + (tp - 2) * (1 + beside)

    def spread(round_):
        far = window << round_
        for there, peer in ((me >= far, me - far), (me + far < n, me + far)):
            pl.when(there)(functools.partial(
                pl.semaphore_signal, word.at[round_], inc=1, device_id=(peer, mt), device_id_type=MESH
            ))

    def heard(round_):
        far = window << round_
        pl.semaphore_wait(word.at[round_], (me >= far).astype(jnp.int32) + (me + far < n).astype(jnp.int32))

    loads = [pltpu.make_async_copy(w_hbm.at[j], wbuf.at[j], w_sem.at[j]) for j in range(3)]
    for copy in inputs[:3]:
        copy.wait()

    def plan(c):
        below = moved_ref[1, lax.rem(c + n - 1, n)]
        above = moved_ref[0, lax.rem(c + 1, n)]
        start = first_ref[c]
        end = jnp.where(c == n - 1, total, first_ref[lax.rem(c + 1, n)])
        return start, end, below, above, moved_ref[0, c], moved_ref[1, c]

    def numbers(c, rank):
        start, end, below, above, low, high = plan(c)
        return jnp.where(
            rank < below,
            start - below + rank,
            jnp.where(rank >= rows - above, end + rank - (rows - above), start + low + rank - below),
        )

    start, end, below, above, low, high = plan(me)
    count = end - start
    rank = lax.broadcasted_iota(jnp.int32, (2 * rows, 1), 0)
    own_rank = rank - 2 * half
    own_local = jnp.where((own_rank >= below) & (own_rank < rows - above), low + own_rank - below, -1)
    up = jnp.where(rank - half < high, count - high + rank - half, -1)
    wanted = jnp.where(rank < half, rank - half + low, jnp.where(rank < 2 * half, up, own_local))
    pob = pob_ref[...]
    member = (pob == wanted).astype(f32)
    lengths = jnp.maximum(jnp.sum(member, axis=1, keepdims=True), 1.0)
    inputs[3].wait()
    for j in (1, 2, 0):
        loads[j].start()
    means = (
        jnp.dot(member.astype(bf), bytes_ref[...], preferred_element_type=f32) / lengths
    ).astype(bf)
    blk[0] = means[:half]
    blk[1] = means[half : 2 * half]

    @pl.when(me == 0)
    def _():
        came[1] = jnp.zeros_like(came[1])
        lo_part[...] = jnp.zeros_like(lo_part)

    @pl.when(me == n - 1)
    def _():
        came[0] = jnp.zeros_like(came[0])
        hi_part[...] = jnp.zeros_like(hi_part)

    pl.semaphore_wait(barrier, expected)
    to_left = remote(blk.at[0], came.at[0], send_nb.at[0], recv_nb.at[0], (left, mt))
    to_right = remote(blk.at[1], came.at[1], send_nb.at[1], recv_nb.at[1], (right, mt))
    pl.when(has_left)(to_left.start)
    pl.when(has_right)(to_right.start)
    spread(0)
    heard(0)
    spread(1)

    def amount(count):
        return tally.at[pl.ds(0, count)]

    def came_in(sem, count):
        remote(amount(count), amount(count), sem, sem, mate).wait_recv()

    def went_out(sem, count):
        remote(amount(count), amount(count), sem, sem, mate).wait_send()

    def but_own(wait, sem, count, own=1):
        pl.when(at_home)(lambda: wait(sem, count - own))
        pl.when(jnp.logical_not(at_home))(lambda: wait(sem, count))

    def start_each(lo, hi, make):
        def act(i):
            other, copy = make(i)
            pl.when(other != me)(copy.start)

        each(lo, hi, act)

    def send_block(a, ref, out):
        def make(i):
            chip = 2 * i + sub
            return chip, remote(
                ref.at[:, cols(i // groups)], out.at[place, parity], sent.at[0], recv_x.at[a],
                (chip, base + parity),
            )

        return make

    def send_query(a, ref, out):
        def make(h):
            chip = 2 * (h * groups + my_group) + sub
            return chip, remote(
                ref.at[:, cols(h)], out.at[slot], sent.at[0],
                recv_q.at[slot // block] if a == 2 else recv_x.at[2], (chip, base + parity),
            )

        return make

    def forward(a, ref):
        return remote(ref.at[:, sub], ref.at[:, sub], sent.at[0], recv_f.at[a], mate)

    def back_query(a, ref, out):
        def make(j):
            c = j * stride + offset
            return c, remote(
                ref.at[j], out.at[:, cols(my_head)], sent.at[0], recv_o.at[a], (c, source_tp)
            )

        return make

    def back_block(i):
        c = 2 * i + sub
        return c, remote(
            dkv.at[:, i, sub], dkv_in.at[:, my_group, :, cols(my_head)], sent.at[0],
            recv_b.at[my_head // per], (c, source_tp),
        )

    send_g, send_q = send_query(3, d_ref, gb), send_query(2, own3.at[0], qb)
    send_k, send_v = send_block(0, own3.at[1], kb), send_block(1, own3.at[2], vb)
    upper = me >= n // 2
    lower = jnp.logical_not(upper)
    early = chunks // 2

    def send_gradients(places):
        for s in places:
            start_each(order(s) * per, order(s) * per + per, send_g)

    @pl.when(upper)
    def _():
        heard(1)
        inputs[4].wait()
        send_gradients(range(early))

    lane = lax.broadcasted_iota(jnp.int32, (1, total), 1)

    def number_keys(c, ids):
        return jnp.where((lane >= c * rows) & (lane < (c + 1) * rows), numbers(c, lane - c * rows), ids)

    kid = lax.fori_loop(0, n, number_keys, jnp.zeros((1, total), jnp.int32))
    pl.when(has_left)(to_right.wait_recv)
    pl.when(has_right)(to_left.wait_recv)
    pooled[pl.ds(0, half)] = means[2 * half : 3 * half] + came[1]
    pooled[pl.ds(half, half)] = means[3 * half :] + came[0]
    mine = cols(my_head)
    makers = (send_q, send_k, send_v)

    for j in (1, 2, 0):
        loads[j].wait()

    def project(kinds):
        for j, places in kinds:
            for s in places:
                span = cols(order(s) * per, per)
                own3[j, :, span] = jnp.dot(
                    pooled[...], wbuf[j, :, span], preferred_element_type=f32
                ).astype(bf)
                if j == 1 and s == 0:
                    pl.when(lower)(functools.partial(heard, 1))
                each_head = per if j == 0 else per * groups
                start_each(order(s) * each_head, (order(s) + 1) * each_head, makers[j])

    outer = (me < n // 4) | (me >= n - n // 4)
    far_first = list(range(chunks))
    distant, close = far_first[:early], far_first[early:]
    project(((1, distant), (2, distant)))
    pl.when(outer)(lambda: project(((0, distant), (1, close), (2, close), (0, close))))
    pl.when(jnp.logical_not(outer))(lambda: project(((1, close), (2, close), (0, close), (0, distant))))

    @pl.when(lower)
    def _():
        inputs[4].wait()
        send_gradients(range(early))

    send_gradients(range(early, chunks))

    @pl.when(parity == sub)
    def _():
        qb[slot] = own3[0, :, mine]
        kb[place, parity] = own3[1, :, mine]
        vb[place, parity] = own3[2, :, mine]
        gb[slot] = d_ref[:, mine]

    over_last = (((1,), (1,)), ((), ()))
    over_first = (((0,), (0,)), ((), ()))
    back_o, back_q = back_query(0, ob, o_in), back_query(1, dqb, dq_in)
    row = lax.broadcasted_iota(jnp.int32, (rows, 1), 0)
    step_keys = max(2, 128 // rows)

    def reach_of(b):
        if b < 0:
            return 0
        reach = min(n, (b + 1) * block * stride + 1)
        return min(n, -(-reach // step_keys) * step_keys)

    def at(c):
        return pl.ds(pl.multiple_of(c * rows, rows), rows)

    def settled_sum(a, c):
        value = dkva[at(c), a * HD : (a + 1) * HD]
        return value * scale if a == 0 else value

    def hand_over(step, lo, hi):
        def act(i):
            for a in range(2):
                dkv[a, i, 1 - sub] = settled_sum(a, 2 * i + 1 - sub).astype(bf)

        each(lo // 2, hi // 2, act)
        span = pl.ds(lo // 2, (hi - lo) // 2)
        remote(dkv.at[:, span, 1 - sub], xkv.at[:, span], sent.at[0], recv_m.at[step], mate).start()

    def send_home(step, lo, hi):
        came_in(recv_m.at[step], hi - lo)

        def act(i):
            for a in range(2):
                dkv[a, i, sub] = (settled_sum(a, 2 * i + sub) + xkv[a, i].astype(f32)).astype(bf)
            other, copy = back_block(i)
            pl.when(other != me)(copy.start)

        each(lo // 2, hi // 2, act)

    steps = list(reversed(range(heads // block)))
    but_own(came_in, recv_x.at[0], pairs)
    forward(0, kb).start()
    for j in (1, 2):
        wt[j - 1] = wbuf[j].T
    but_own(came_in, recv_x.at[1], pairs)
    forward(1, vb).start()
    came_in(recv_f.at[0], pairs)

    def weigh(b):
        lo, reach = b * block, reach_of(b)
        keys = reach * rows
        q = qb[pl.ds(lo, block)].reshape(block * rows, HD)
        k = kb[pl.ds(0, reach // 2)].reshape(keys, HD)
        qid = jnp.concatenate([numbers((lo + j) * stride + offset, row) for j in range(block)], axis=0)
        allowed = qid >= kid[:, :keys]
        score = lax.dot_general(q, k, over_last, preferred_element_type=f32) * scale
        score = jnp.where(allowed, score, -jnp.inf)
        top = jnp.max(score, axis=1, keepdims=True)
        e = jnp.exp(score - top)
        pa[b, :, pl.ds(0, keys)] = e * (1.0 / jnp.sum(e, axis=1, keepdims=True))

    def attend(b):
        lo = b * block
        keys = reach_of(b) * rows
        v = vb[pl.ds(0, reach_of(b) // 2)].reshape(keys, HD)
        out = jnp.dot(pa[b, :, pl.ds(0, keys)].astype(bf), v, preferred_element_type=f32).astype(bf)
        ob[pl.ds(lo, block)] = out.reshape(block, rows, HD)

    def differentiate(b, filled):
        lo = b * block
        keys = reach_of(b) * rows
        q = qb[pl.ds(lo, block)].reshape(block * rows, HD)
        g = gb[pl.ds(lo, block)].reshape(block * rows, HD)
        k = kb[pl.ds(0, reach_of(b) // 2)].reshape(keys, HD)
        v = vb[pl.ds(0, reach_of(b) // 2)].reshape(keys, HD)
        out = ob[pl.ds(lo, block)].reshape(block * rows, HD)
        prob = pa[b, :, pl.ds(0, keys)]
        delta = jnp.sum(g.astype(f32) * out.astype(f32), axis=1, keepdims=True)
        dprob = lax.dot_general(g, v, over_last, preferred_element_type=f32)
        dscore = (prob * (dprob - delta)).astype(bf)
        dq = (jnp.dot(dscore, k, preferred_element_type=f32) * scale).astype(bf)
        dqb[pl.ds(lo, block)] = dq.reshape(block, rows, HD)
        blank = jnp.zeros_like(q)
        both = lax.dot_general(
            jnp.concatenate([dscore, prob.astype(bf)], axis=0),
            jnp.concatenate(
                [jnp.concatenate([q, blank], axis=1), jnp.concatenate([blank, g], axis=1)], axis=0
            ),
            over_first, preferred_element_type=f32,
        )
        old = min(keys, filled)
        if old:
            dkva[pl.ds(0, old)] += both[:old]
        if keys > old:
            dkva[pl.ds(old, keys - old)] = both[old:]
        return max(keys, filled)

    middle = n // 2 // step_keys * step_keys
    whole = [(i, lo, hi) for i, (lo, hi) in enumerate(((0, middle), (middle, n))) if hi > lo]
    falling = (steps, {b: [(b, reach_of(b - 1), reach_of(b))] for b in steps if reach_of(b) > reach_of(b - 1)})
    rising = (steps[::-1], {steps[0]: whole})
    halves = [(upper, rising), (lower, falling)] if len(steps) > 1 else [(me >= 0, falling)]

    def work(blocks, spans):
        lead, first = max(1, len(blocks) // 2), blocks[:1]
        for part_of in (first, blocks[1:lead], blocks[lead:]):
            for b in part_of:
                mine_too = at_home & (slot // block == b)
                pl.when(mine_too)(lambda: came_in(recv_q.at[b], block - 1))
                pl.when(jnp.logical_not(mine_too))(lambda: came_in(recv_q.at[b], block))
            for b in part_of:
                weigh(b)
            if part_of is first:
                came_in(recv_f.at[1], pairs)
            for b in part_of:
                attend(b)
            for b in part_of:
                start_each(b * block, (b + 1) * block, back_o)
        but_own(came_in, recv_x.at[2], heads)
        late, filled = [], 0
        for part_of in (blocks[:lead], blocks[lead:]):
            for b in part_of:
                filled = differentiate(b, filled)
            for b in part_of:
                start_each(b * block, (b + 1) * block, back_q)
            ready = [span for b in part_of for span in spans.get(b, ())]
            for span in ready:
                hand_over(*span)
            for span in late:
                send_home(*span)
            late = ready
        for span in late:
            send_home(*span)

    for here, plan_of in halves:
        pl.when(here)(functools.partial(work, *plan_of))

    @pl.when(parity == sub)
    def _():
        o_in[:, mine] = ob[slot]
        dq_in[:, mine] = dqb[slot]
        for a in range(2):
            dkv_in[a, my_group, :, mine] = dkv[a, place, parity]

    but_own(came_in, recv_o.at[0], heads)
    attn_ref[...] = o_in[...]
    but_own(came_in, recv_o.at[1], heads)
    partial = lax.dot_general(dq_in[...], wbuf[0], over_last, preferred_element_type=f32)
    for s in reversed(range(chunks)):
        chunk = order(s)
        span = cols(chunk * per, per)
        blocks = 2 * per * groups
        own_chunk = at_home & (chunk == my_head // per)
        pl.when(own_chunk)(lambda: came_in(recv_b.at[chunk], blocks - 2))
        pl.when(jnp.logical_not(own_chunk))(lambda: came_in(recv_b.at[chunk], blocks))
        for j in (1, 2):
            if groups == 1:
                summed = dkv_in[j - 1, 0, :, span]
            else:
                summed = dkv_in[j - 1, 0, :, span].astype(f32)
                for i in range(1, groups):
                    summed = summed + dkv_in[j - 1, i, :, span].astype(f32)
                summed = summed.astype(bf)
            partial += jnp.dot(summed, wt[j - 1, span], preferred_element_type=f32)
    for t in range(tp):
        part[t] = partial[:, t * width : (t + 1) * width].astype(bf)
    edge_lo, edge_hi = pl.ds(0, half), pl.ds(rows - half, half)
    def give_back(a, piece, into, peer):
        return [
            remote(piece(t), into.at[mt], send_r.at[a], recv_r.at[a], (peer, t))
            for t in (lax.rem(mt + i, tp) for i in range(1 if a == 2 else 0, tp))
        ]

    @pl.when(has_left)
    def _():
        for copy in give_back(0, lambda t: part.at[t, edge_lo], hi_part, left):
            copy.start()

    @pl.when(has_right)
    def _():
        for copy in give_back(1, lambda t: part.at[t, edge_hi], lo_part, right):
            copy.start()

    for copy in give_back(2, lambda t: part.at[t], own_part, me):
        copy.start()
    own_part[mt] = part[mt]
    target = jnp.where(
        pob < low,
        half - low + pob,
        jnp.where(pob >= count - high, half + rows + pob - (count - high), half + below + pob - low),
    )
    chooser = (target == lax.broadcasted_iota(jnp.int32, (2 * rows, 1), 0)).astype(f32)
    sizes = jnp.maximum(jnp.sum(chooser, axis=1, keepdims=True), 1.0)
    pl.when(has_left)(to_left.wait_send)
    pl.when(has_right)(to_right.wait_send)
    but_own(went_out, sent.at[0], 8 * pairs + 4 * heads, 8)
    others = own_part.at[pl.ds(0, tp - 1)]
    for here, a, ref in ((has_right, 0, hi_part), (has_left, 1, lo_part)):
        pl.when(here)(lambda: remote(ref, ref, send_r.at[a], recv_r.at[a], mate).wait_recv())
    remote(others, others, send_r.at[2], recv_r.at[2], mate).wait_recv()
    for here, a, ref in ((has_left, 0, hi_part), (has_right, 1, lo_part)):
        pl.when(here)(lambda: remote(ref, ref, send_r.at[a], recv_r.at[a], mate).wait_send())
    remote(others, others, send_r.at[2], recv_r.at[2], mate).wait_send()

    def over_tp(ref):
        value = ref[0].astype(f32)
        for i in range(1, tp):
            value = value + ref[i].astype(f32)
        return value

    returned = jnp.concatenate([over_tp(lo_part), over_tp(own_part), over_tp(hi_part)], axis=0)
    shares = (returned.astype(bf).astype(f32) / sizes).astype(bf)
    grad_ref[...] = lax.dot_general(
        chooser.astype(bf), shares, over_first, preferred_element_type=f32
    ).astype(bf)


def emit_kernel(a_ref, g_ref, a_out, g_out, sem):
    copies = [
        pltpu.make_async_copy(src, dst, sem.at[i]) for i, (src, dst) in enumerate(((a_ref, a_out), (g_ref, g_out)))
    ]
    for copy in copies:
        copy.start()
    for copy in copies:
        copy.wait()


def shards(byte_states, patch_of_byte, patch_first, moved, w_qkv, d_attn):
    n, tp = lax.axis_size("ctx"), lax.axis_size("tp")
    rows, feats = d_attn.shape
    size, model = byte_states.shape
    heads = feats // HD
    pairs = n // 2
    groups = pairs // heads
    total = n * rows
    half = rows // 2
    width = model // tp
    block = per = 2 if heads % 2 == 0 else 1
    steps = heads // block
    assert tp % 2 == 0 and n % 2 == 0 and pairs % heads == 0
    bf, f32, i32 = jnp.bfloat16, jnp.float32, jnp.int32
    dma = pltpu.SemaphoreType.DMA
    results = pl.pallas_call(
        functools.partial(whole_kernel, n, tp, heads, rows, block, per),
        out_shape=[pltpu.VMEM((rows, feats), bf), pltpu.VMEM((size, width), bf)],
        in_specs=[ANY] * 6,
        out_specs=[VM] * 2,
        scratch_shapes=[
            pltpu.VMEM((size, model), bf), pltpu.VMEM((1, size), i32),
            pltpu.SMEM((n,), i32), pltpu.SMEM((2, n), i32),
            pltpu.VMEM(w_qkv.shape, bf), pltpu.VMEM((rows, feats), bf),
            pltpu.VMEM((2, half, model), bf), pltpu.VMEM((2, half, model), bf),
            pltpu.VMEM((rows, model), bf), pltpu.VMEM((3, rows, feats), bf),
            pltpu.VMEM((heads, rows, HD), bf), pltpu.VMEM((heads, rows, HD), bf),
            pltpu.VMEM((pairs, 2, rows, HD), bf), pltpu.VMEM((pairs, 2, rows, HD), bf),
            pltpu.VMEM((steps, block * rows, total), f32),
            pltpu.VMEM((heads, rows, HD), bf), pltpu.VMEM((heads, rows, HD), bf),
            pltpu.VMEM((2, pairs, 2, rows, HD), bf), pltpu.VMEM((2, pairs, rows, HD), bf),
            pltpu.VMEM((total, 2 * HD), f32), pltpu.VMEM((2, feats, model), bf),
            pltpu.VMEM((rows, feats), bf), pltpu.VMEM((rows, feats), bf),
            pltpu.VMEM((2, groups, rows, feats), bf),
            pltpu.VMEM((tp, rows, width), bf), pltpu.VMEM((tp, rows, width), bf),
            pltpu.VMEM((tp, half, width), bf), pltpu.VMEM((tp, half, width), bf),
            pltpu.VMEM((8 * pairs + 4 * heads, rows, HD), bf),
            dma((5,)), dma((3,)), dma((2,)), dma((2,)), dma((1,)), dma((3,)), dma((steps,)), dma((2,)),
            dma((max(2, steps),)), dma((2,)), dma((heads // per,)), dma((3,)), dma((3,)),
            pltpu.SemaphoreType.REGULAR((2,)),
        ],
        compiler_params=pltpu.CompilerParams(
            collective_id=0, has_side_effects=True, vmem_limit_bytes=60 << 20
        ),
        name="whole",
    )(byte_states, patch_of_byte.reshape(1, size), patch_first, moved, w_qkv, d_attn)
    results = [pltpu.with_memory_space_constraint(x, pltpu.VMEM) for x in results]
    return tuple(pl.pallas_call(
        emit_kernel,
        out_shape=[jax.ShapeDtypeStruct((rows, feats), bf), jax.ShapeDtypeStruct((size, width), bf)],
        in_specs=[VM, VM],
        out_specs=[ANY] * 2,
        scratch_shapes=[dma((2,))],
        name="emit",
    )(*results))


def solution(mesh):
    placed = (P("ctx", None), P("ctx"), P(), P(), P(None, None, "tp"), P("ctx", "tp"))
    return jax.shard_map(
        shards,
        mesh=mesh,
        in_specs=placed,
        out_specs=(P("ctx", "tp"), P("ctx", "tp")),
        check_vma=False,
    )
```
